256 devices in a mesh: ang: 32 (over y, z_lo, core), sl: 8 (over z_hi, x).
Axes of the slice: x: 4, y: 4, z: 8 (z_hi: 2, z_lo: 4; z = z_hi * 4 + z_lo), core: 2. Of those that a mesh axis runs over, the one named last changes fastest.
Arguments:
- sinogram: bfloat16 [64, 64, 1024], P('sl', 'ang'), may hold values from -72 to 72
- detector_coord: int32 [64, 64, 512], P('ang', 'sl'), may hold values from 0 to 1072693247
Outputs:
- image_rows: float32 [64, 64, 512], P('ang', 'sl')
The draws below stay inside these ranges and needn't reach their ends.
All inputs are finite; a program needn't handle non-finite values.
Results may differ from the reference program's by a relative error of at most 0.0052.
Values may be sent and summed in bfloat16 or wider, within the bound.
No kernel may reach another device: no remote copies, remote signals or barrier semaphores. Data moves between devices by JAX's collectives and lax.ppermute only.
A program may use at most 64 MiB of HBM per device.

```python
import math
import jax
import jax.numpy as jnp
from jax import lax

BINS = 1024
IMG = 512
SLICES = 64
ANGLES = 64
ROWS = 64


def place_ends(result, own_key, least, high):
    index_at = [jax.random.randint(jax.random.fold_in(own_key, axis), (), 0, length) for axis, length in enumerate(result.shape)]
    longest = result.shape.index(max(result.shape))
    beside = index_at[:longest] + [(index_at[longest] + 1) % result.shape[longest]] + index_at[longest + 1:]
    return result.at[tuple(index_at)].set(least).at[tuple(beside)].set(high)


def levels(key, shape, split, low, high):
    gain, own = 1.0, jax.random.fold_in(key, 6)
    for dim, parts in split:
        heights = jnp.exp(jax.random.uniform(jax.random.fold_in(own, dim), (parts,), jnp.float32, low / len(split), high / len(split)))
        gain = gain * jnp.repeat(heights, shape[dim] // parts).reshape([-1 if axis == dim else 1 for axis in range(len(shape))])
    return gain


def bell_draw(rng, dims, scale, reach, shards=(), kind=jnp.bfloat16):
    values = scale * jax.random.normal(rng, dims, jnp.float32)
    if shards:
        values = values * levels(rng, dims, shards, -0.22, 0.18)
    return jnp.clip(values, -reach, reach).astype(kind)


def setup_inputs(seed: int = 0) -> dict:
    key_list = jax.random.split(jax.random.key(seed), 3)
    return {
        "sinogram": bell_draw(key_list[0], (SLICES, ANGLES, BINS), 12.0, 72.0, ((0, 8), (1, 32))),
        "detector_coord": place_ends(jax.random.randint(key_list[1], (ANGLES, ROWS, IMG), 0, (BINS - 1) * 1048576), jax.random.fold_in(key_list[1], 1), 0, ((BINS - 1) * 1048576) - 1).astype(jnp.int32),
    }


def ramp_table(bin_count):
    first = lax.broadcasted_iota(jnp.int32, (bin_count, bin_count), 0)
    second = lax.broadcasted_iota(jnp.int32, (bin_count, bin_count), 1)
    offset = second - first
    offset_sq = jnp.maximum((offset * offset).astype(jnp.float32), jnp.float32(1.0))
    odd_mask = (offset % 2) != 0
    values = jnp.where(offset == 0, jnp.float32(0.25), jnp.where(odd_mask, jnp.float32(-1.0 / (math.pi ** 2)) / offset_sq, jnp.float32(0.0)))
    return values.astype(jnp.bfloat16)


def interp_weights(row_coords, bin_count):
    bin_left = row_coords // 1048576
    fraction = (row_coords % 1048576).astype(jnp.float32) / jnp.float32(1048576.0)
    positions = lax.broadcasted_iota(jnp.int32, row_coords.shape + (bin_count,), 2)
    left_part = jnp.where(positions == bin_left[..., None], 1.0 - fraction[..., None], jnp.float32(0.0))
    right_part = jnp.where(positions == bin_left[..., None] + 1, fraction[..., None], jnp.float32(0.0))
    return (left_part + right_part).astype(jnp.bfloat16)


def reference(sinogram, detector_coord):
    slices, angles, bin_count = sinogram.shape
    table = ramp_table(bin_count)
    filtered = jnp.dot(sinogram.reshape(slices * angles, bin_count), table, preferred_element_type=jnp.float32)
    filtered = filtered.astype(jnp.bfloat16).reshape(slices, angles, bin_count)

    def add_angle(running, angle_step):
        projection = lax.dynamic_index_in_dim(filtered, angle_step, 1, keepdims=False)
        row_coords = lax.dynamic_index_in_dim(detector_coord, angle_step, 0, keepdims=False)
        weights = interp_weights(row_coords, bin_count)
        contrib = jnp.einsum('rxb,sb->rsx', weights.astype(jnp.float32), projection.astype(jnp.float32))
        return running + contrib, None

    start_value = jnp.zeros((detector_coord.shape[1], slices, detector_coord.shape[2]), jnp.float32)
    running, unused = lax.scan(add_angle, start_value, jnp.arange(angles, dtype=jnp.int32))
    return running * jnp.float32(math.pi / angles)
```

```python
import math

import jax
import jax.numpy as jnp
from jax import lax
from jax.experimental import pallas as pl
from jax.experimental.pallas import tpu as pltpu
from jax.sharding import Mesh
from jax.sharding import PartitionSpec as P

SLICE_ORDER = (0, 2, 4, 6, 1, 3, 5, 7)
LANES = 128
LANE_DIMS = lax.GatherDimensionNumbers(
    offset_dims=(),
    collapsed_slice_dims=(1,),
    start_index_map=(1,),
    operand_batching_dims=(0,),
    start_indices_batching_dims=(0,),
)


def ramp_table(bin_count):
    first = lax.broadcasted_iota(jnp.int32, (bin_count, bin_count), 0)
    second = lax.broadcasted_iota(jnp.int32, (bin_count, bin_count), 1)
    offset = second - first
    offset_sq = jnp.maximum((offset * offset).astype(jnp.float32), jnp.float32(1.0))
    odd_mask = offset % 2 != 0
    values = jnp.where(
        offset == 0,
        jnp.float32(0.25),
        jnp.where(odd_mask, jnp.float32(-1.0 / math.pi**2) / offset_sq, jnp.float32(0.0)),
    )
    return values.astype(jnp.bfloat16)


def lane_gather(table, lanes):
    return lax.gather(
        table, lanes[..., None], LANE_DIMS, (1, 1), mode=lax.GatherScatterMode.PROMISE_IN_BOUNDS
    )


def project_kernel(place, tab, *refs):
    coords, (out, tab_s, left_s, w1_s, w2_s) = refs[:8], refs[8:]
    tab_s[...] = tab[...]
    even = lax.broadcasted_iota(jnp.int32, (8, LANES), 0) % 2 == 0
    for n in range(8):
        for core in range(2):
            c = coords[n][core]
            fraction = (c & 1048575).astype(jnp.float32) * jnp.float32(1.0 / 1048576.0)
            left_s[n, core] = c >> 20
            w1_s[n, core] = (1.0 - fraction).astype(jnp.bfloat16).astype(jnp.float32)
            w2_s[n, core] = fraction.astype(jnp.bfloat16).astype(jnp.float32)

    def one_tile(step, carry):
        n = step // 4
        lanes_at = pl.ds(pl.multiple_of((step % 4) * LANES, LANES), LANES)
        owner = place[n]
        for pair in range(2):
            for row in range(2):
                acc_even = acc_odd = None
                for core in range(2):
                    for angle in range(2):
                        i = angle * 4 + pair * 2 + row
                        left = jnp.broadcast_to(left_s[n, core, i : i + 1, lanes_at], (16, LANES))
                        left = left.astype(jnp.int16)
                        low = left & jnp.int16(LANES - 1)
                        taps = [
                            lane_gather(tab_s[core * 2 + angle, :, k * LANES : (k + 1) * LANES], low)
                            for k in range(8)
                        ]
                        for bit in (128, 256, 512):
                            high = (left & jnp.int16(bit)) != 0
                            taps = [
                                jnp.where(high, taps[k + 1], taps[k]) for k in range(0, len(taps), 2)
                            ]
                        both = taps[0].astype(jnp.float32)
                        weight = jnp.where(
                            even,
                            jnp.broadcast_to(w1_s[n, core, i : i + 1, lanes_at], (8, LANES)),
                            jnp.broadcast_to(w2_s[n, core, i : i + 1, lanes_at], (8, LANES)),
                        )
                        part_even, part_odd = both[:8] * weight, both[8:] * weight
                        acc_even = part_even if acc_even is None else acc_even + part_even
                        acc_odd = part_odd if acc_odd is None else acc_odd + part_odd
                total = jnp.where(
                    even, acc_even + pltpu.roll(acc_even, 7, 0), acc_odd + pltpu.roll(acc_odd, 1, 0)
                )
                out[2 * owner + pair, row * 8 : (row + 1) * 8, lanes_at] = total.astype(out.dtype)
        return carry

    lax.fori_loop(0, 32, one_tile, 0)


def project(place, tab, coords):
    vmem = pl.BlockSpec(memory_space=pltpu.VMEM)
    return pl.pallas_call(
        project_kernel,
        out_shape=jax.ShapeDtypeStruct((16, 16, 512), jnp.bfloat16),
        in_specs=[pl.BlockSpec(memory_space=pltpu.SMEM), vmem] + [vmem] * 8,
        out_specs=vmem,
        scratch_shapes=[
            pltpu.VMEM((4, 16, 1024), jnp.bfloat16),
            pltpu.VMEM((8, 2, 8, 512), jnp.int32),
            pltpu.VMEM((8, 2, 8, 512), jnp.float32),
            pltpu.VMEM((8, 2, 8, 512), jnp.float32),
        ],
        name="project",
    )(place, tab, *coords)


def shards(sinogram, detector_coord):
    slices, angles, bins = sinogram.shape
    width = detector_coord.shape[2]
    core, z_high, x = lax.axis_index("core"), lax.axis_index("z_hi"), lax.axis_index("x")
    swap = [(0, 1), (1, 0)]

    by_core = detector_coord.reshape(angles, 2, 2, 2, width)
    keep = lax.dynamic_index_in_dim(by_core, core, 2, keepdims=False).reshape(8, width)
    give = lax.dynamic_index_in_dim(by_core, 1 - core, 2, keepdims=False).reshape(8, width)
    own = jnp.stack([keep, lax.ppermute(give, "core", swap)])
    other = lax.ppermute(own, "z_hi", swap)

    def from_x(array, step):
        return lax.ppermute(array, "x", [((i + step) % 4, i) for i in range(4)])

    coords = [own] + [from_x(own, s) for s in (1, 2, 3)]
    coords += [other] + [from_x(other, s) for s in (1, 2, 3)]
    places = [4 * z + (x + s) % 4 for z in (z_high, 1 - z_high) for s in range(4)]
    place = jnp.stack(places).astype(jnp.int32)

    other_sino = lax.ppermute(sinogram, "core", swap)
    rows = jnp.stack([sinogram, other_sino]).transpose(0, 2, 1, 3)[:, :, SLICE_ORDER, :]
    filtered = jnp.dot(
        rows.reshape(4 * slices, bins), ramp_table(bins), preferred_element_type=jnp.float32
    ).astype(jnp.bfloat16)
    ahead = jnp.concatenate([filtered[:, 1:], filtered[:, :1]], axis=1)
    tab = jnp.stack([filtered, ahead], axis=1).reshape(4, 16, bins)

    partial = project(place, tab, coords)
    parts = lax.all_to_all(partial, ("y", "z_lo"), 0, 0, tiled=True)
    scale = jnp.float32(math.pi / (angles * lax.axis_size(("y", "z_lo", "core"))))
    image_rows = jnp.sum(parts.astype(jnp.float32), axis=0) * scale
    return image_rows.reshape(2, slices, width)


def solution(mesh):
    names = ("y", "z_lo", "core", "z_hi", "x")
    fine = Mesh(mesh.devices.reshape(4, 4, 2, 2, 4), names)
    ang, sl = ("y", "z_lo", "core"), ("z_hi", "x")
    in_specs = (P(sl, ang, None), P(ang, sl, None))
    return jax.shard_map(
        shards, mesh=fine, in_specs=in_specs, out_specs=P(ang, sl, None), check_vma=False
    )
```

```python
import math

import jax
import jax.numpy as jnp
from jax import lax
from jax.experimental import pallas as pl
from jax.experimental.pallas import tpu as pltpu
from jax.sharding import Mesh
from jax.sharding import PartitionSpec as P

LANES = 128
LANE_DIMS = lax.GatherDimensionNumbers(
    offset_dims=(),
    collapsed_slice_dims=(1,),
    start_index_map=(1,),
    operand_batching_dims=(0,),
    start_indices_batching_dims=(0,),
)
VMEM = pl.BlockSpec(memory_space=pltpu.VMEM)


def lane_gather(table, lanes):
    return lax.gather(
        table, lanes[..., None], LANE_DIMS, (1, 1), mode=lax.GatherScatterMode.PROMISE_IN_BOUNDS
    )


def filter_kernel(own, other, out, strip):
    bins = own.shape[1]
    blocks = bins // LANES
    for j in range(2 * blocks - 1):
        first = lax.broadcasted_iota(jnp.int32, (LANES, LANES), 0)
        second = lax.broadcasted_iota(jnp.int32, (LANES, LANES), 1)
        offset = second - first + (j - blocks + 1) * LANES
        offset_sq = jnp.maximum((offset * offset).astype(jnp.float32), jnp.float32(1.0))
        values = jnp.where(
            (offset & 1) != 0, jnp.float32(-1.0 / math.pi**2) / offset_sq, jnp.float32(0.0)
        )
        if j == blocks - 1:
            values = jnp.where(offset == 0, jnp.float32(0.25), values)
        strip[:, j * LANES : (j + 1) * LANES] = values.astype(jnp.bfloat16)
    rows = jnp.concatenate([own[...], other[...]], axis=0)
    total = None
    for k in range(blocks):
        start = (blocks - 1 - k) * LANES
        part = jnp.dot(
            rows[:, k * LANES : (k + 1) * LANES],
            strip[:, start : start + bins],
            preferred_element_type=jnp.float32,
        )
        total = part if total is None else total + part
    out[...] = total.astype(jnp.bfloat16).astype(jnp.float32)


def filter_rows(own, other):
    rows, bins = own.shape
    return pl.pallas_call(
        filter_kernel,
        out_shape=jax.ShapeDtypeStruct((2 * rows, bins), jnp.float32),
        in_specs=[VMEM, VMEM],
        out_specs=VMEM,
        scratch_shapes=[pltpu.VMEM((LANES, 2 * bins - LANES), jnp.bfloat16)],
        compiler_params=pltpu.CompilerParams(vmem_limit_bytes=8 * 2**20),
        name="filter_rows",
    )(own, other)


def transposed(tiles):
    sublane = lax.broadcasted_iota(jnp.int32, (8, LANES), 0)
    for step in (4, 2, 1):
        low = (sublane & step) == 0
        done = list(tiles)
        for i in range(8):
            if not i & step:
                a, b = tiles[i], tiles[i + step]
                done[i] = jnp.where(low, a, pltpu.roll(b, step, 0))
                done[i + step] = jnp.where(low, pltpu.roll(a, 8 - step, 0), b)
        tiles = done
    return tiles


def project_half(tab, coords, out, base):
    x = lax.axis_index("x")
    sublane = lax.broadcasted_iota(jnp.int32, (8, LANES), 0)

    def one_tile(step):
        two, at = step // 4, pl.ds(pl.multiple_of((step % 4) * LANES, LANES), LANES)
        sums = [None] * 8
        for core in range(2):
            first, second = coords[2 * two, core, :, at], coords[2 * two + 1, core, :, at]
            for angle in range(2):
                if angle == 0:
                    c = jnp.where(sublane < 4, first, pltpu.roll(second, 4, 0))
                else:
                    c = jnp.where(sublane < 4, pltpu.roll(first, 4, 0), second)
                left = c >> 20
                fraction = (c & 1048575).astype(jnp.float32) * jnp.float32(1.0 / 1048576.0)
                w_left = (1.0 - fraction).astype(jnp.bfloat16).astype(jnp.float32)
                w_right = fraction.astype(jnp.bfloat16).astype(jnp.float32)
                bins = jnp.concatenate([left, left + 1], axis=0).astype(jnp.int16)
                lanes = bins & jnp.int16(LANES - 1)
                high = [(bins & jnp.int16(bit)) != 0 for bit in (128, 256, 512)]
                for s in range(8):
                    row = core * 16 + s * 2 + angle
                    taps = []
                    for k in range(8):
                        source = jnp.broadcast_to(
                            tab[row : row + 1, k * LANES : (k + 1) * LANES], (16, LANES)
                        )
                        taps.append(lane_gather(source.astype(jnp.bfloat16), lanes))
                    for mask in high:
                        taps = [
                            jnp.where(mask, taps[k + 1], taps[k]) for k in range(0, len(taps), 2)
                        ]
                    both = taps[0].astype(jnp.float32)
                    part = both[:8] * w_left + both[8:] * w_right
                    sums[s] = part if sums[s] is None else sums[s] + part
        rows = transposed(sums)
        for i in range(2):
            owner = base + 2 * ((x + 2 * two + i) & 3)
            for pair in range(2):
                for r in range(2):
                    value = rows[i * 4 + pair * 2 + r].astype(out.dtype)
                    out[owner + pair, r * 8 : (r + 1) * 8, at] = value

    def two_tiles(step, carry):
        one_tile(2 * step)
        one_tile(2 * step + 1)
        return carry

    lax.fori_loop(0, 4, two_tiles, 0)


def near_kernel(tab, c0, c1, c2, c3, out, coords):
    for i, c in enumerate((c0, c1, c2, c3)):
        coords[i] = c[...]
    project_half(tab, coords, out, 0)


def far_kernel(tab, c0, c1, c2, c3, near, out, coords):
    for i, c in enumerate((c0, c1, c2, c3)):
        coords[i] = c[...]
    z_high = lax.axis_index("z_hi")
    out[pl.ds(8 * z_high, 8)] = near[...]
    project_half(tab, coords, out, 8 * (1 - z_high))


def project(kernel, owners, operands, name):
    return pl.pallas_call(
        kernel,
        out_shape=jax.ShapeDtypeStruct((owners, 16, 512), jnp.bfloat16),
        in_specs=[VMEM] * len(operands),
        out_specs=VMEM,
        scratch_shapes=[pltpu.VMEM((4, 2, 8, 512), jnp.int32)],
        compiler_params=pltpu.CompilerParams(vmem_limit_bytes=8 * 2**20),
        name=name,
    )(*operands)


def shards(sinogram, detector_coord):
    slices, angles, bins = sinogram.shape
    width = detector_coord.shape[2]
    core = lax.axis_index("core")
    swap = [(0, 1), (1, 0)]

    by_core = detector_coord.reshape(angles, 2, 2, 2, width)
    keep = lax.dynamic_index_in_dim(by_core, core, 2, keepdims=False).reshape(8, width)
    give = lax.dynamic_index_in_dim(by_core, 1 - core, 2, keepdims=False).reshape(8, width)
    own = jnp.stack([keep, lax.ppermute(give, "core", swap)])
    other = lax.ppermute(own, "z_hi", swap)

    def from_x(array, step):
        return lax.ppermute(array, "x", [((i + step) % 4, i) for i in range(4)])

    near = [own] + [from_x(own, s) for s in (1, 2, 3)]
    far = [other] + [from_x(other, s) for s in (1, 2, 3)]

    other_sino = lax.ppermute(sinogram, "core", swap)
    tab = filter_rows(
        sinogram.reshape(slices * angles, bins), other_sino.reshape(slices * angles, bins)
    )
    half = project(near_kernel, 8, [tab, *near], "near")
    partial = project(far_kernel, 16, [tab, *far, half], "far")
    parts = lax.all_to_all(partial, ("y", "z_lo"), 0, 0, tiled=True)
    scale = jnp.float32(math.pi / (angles * lax.axis_size(("y", "z_lo", "core"))))
    image_rows = jnp.sum(parts.astype(jnp.float32), axis=0) * scale
    return image_rows.reshape(2, slices, width)


def solution(mesh):
    names = ("y", "z_lo", "core", "z_hi", "x")
    fine = Mesh(mesh.devices.reshape(4, 4, 2, 2, 4), names)
    ang, sl = ("y", "z_lo", "core"), ("z_hi", "x")
    in_specs = (P(sl, ang, None), P(ang, sl, None))
    return jax.shard_map(
        shards, mesh=fine, in_specs=in_specs, out_specs=P(ang, sl, None), check_vma=False
    )
```

```python
import math

import jax
import jax.numpy as jnp
from jax import lax
from jax.experimental import pallas as pl
from jax.experimental.pallas import tpu as pltpu
from jax.sharding import Mesh
from jax.sharding import PartitionSpec as P

LANES = 128
LANE_DIMS = lax.GatherDimensionNumbers(
    offset_dims=(),
    collapsed_slice_dims=(1,),
    start_index_map=(1,),
    operand_batching_dims=(0,),
    start_indices_batching_dims=(0,),
)
VMEM = pl.BlockSpec(memory_space=pltpu.VMEM)


def lane_gather(table, lanes):
    return lax.gather(
        table, lanes[..., None], LANE_DIMS, (1, 1), mode=lax.GatherScatterMode.PROMISE_IN_BOUNDS
    )


def filter_kernel(own, other, out, strip):
    bins = own.shape[1]
    blocks = bins // LANES
    for j in range(2 * blocks - 1):
        first = lax.broadcasted_iota(jnp.int32, (LANES, LANES), 0)
        second = lax.broadcasted_iota(jnp.int32, (LANES, LANES), 1)
        offset = second - first + (j - blocks + 1) * LANES
        offset_sq = jnp.maximum((offset * offset).astype(jnp.float32), jnp.float32(1.0))
        values = jnp.where(
            (offset & 1) != 0, jnp.float32(-1.0 / math.pi**2) / offset_sq, jnp.float32(0.0)
        )
        if j == blocks - 1:
            values = jnp.where(offset == 0, jnp.float32(0.25), values)
        strip[:, j * LANES : (j + 1) * LANES] = values.astype(jnp.bfloat16)
    rows = jnp.concatenate([own[...], other[...]], axis=0)
    total = None
    for k in range(blocks):
        start = (blocks - 1 - k) * LANES
        part = jnp.dot(
            rows[:, k * LANES : (k + 1) * LANES],
            strip[:, start : start + bins],
            preferred_element_type=jnp.float32,
        )
        total = part if total is None else total + part
    out[...] = total.astype(jnp.bfloat16).astype(jnp.float32)


def filter_rows(own, other):
    rows, bins = own.shape
    return pl.pallas_call(
        filter_kernel,
        out_shape=jax.ShapeDtypeStruct((2 * rows, bins), jnp.float32),
        in_specs=[VMEM, VMEM],
        out_specs=VMEM,
        scratch_shapes=[pltpu.VMEM((LANES, 2 * bins - LANES), jnp.bfloat16)],
        compiler_params=pltpu.CompilerParams(vmem_limit_bytes=8 * 2**20),
        name="filter_rows",
    )(own, other)


def transposed(tiles):
    sublane = lax.broadcasted_iota(jnp.int32, (8, LANES), 0)
    for step in (4, 2, 1):
        low = (sublane & step) == 0
        done = list(tiles)
        for i in range(8):
            if not i & step:
                a, b = tiles[i], tiles[i + step]
                done[i] = jnp.where(low, a, pltpu.roll(b, step, 0))
                done[i + step] = jnp.where(low, pltpu.roll(a, 8 - step, 0), b)
        tiles = done
    return tiles


def project_rows(tab, first_x, second_x, out, places):
    sublane = lax.broadcasted_iota(jnp.int32, (8, LANES), 0)

    def one_tile(step):
        at = pl.ds(pl.multiple_of(step * LANES, LANES), LANES)
        sums = [None] * 8
        for core in range(2):
            first, second = first_x[core, :, at], second_x[core, :, at]
            for angle in range(2):
                if angle == 0:
                    c = jnp.where(sublane < 4, first, pltpu.roll(second, 4, 0))
                else:
                    c = jnp.where(sublane < 4, pltpu.roll(first, 4, 0), second)
                left = c >> 20
                fraction = (c & 1048575).astype(jnp.float32) * jnp.float32(1.0 / 1048576.0)
                w_left = (1.0 - fraction).astype(jnp.bfloat16).astype(jnp.float32)
                w_right = fraction.astype(jnp.bfloat16).astype(jnp.float32)
                bins = jnp.concatenate([left, left + 1], axis=0).astype(jnp.int16)
                lanes = bins & jnp.int16(LANES - 1)
                high = [(bins & jnp.int16(bit)) != 0 for bit in (128, 256, 512)]
                for s in range(8):
                    row = core * 16 + s * 2 + angle
                    taps = []
                    for k in range(8):
                        source = jnp.broadcast_to(
                            tab[row : row + 1, k * LANES : (k + 1) * LANES], (16, LANES)
                        )
                        taps.append(lane_gather(source.astype(jnp.bfloat16), lanes))
                    for mask in high:
                        taps = [
                            jnp.where(mask, taps[k + 1], taps[k]) for k in range(0, len(taps), 2)
                        ]
                    both = taps[0].astype(jnp.float32)
                    part = both[:8] * w_left + both[8:] * w_right
                    sums[s] = part if sums[s] is None else sums[s] + part
        rows = transposed(sums)
        for i in range(2):
            for pair in range(2):
                for r in range(2):
                    value = rows[i * 4 + pair * 2 + r].astype(out.dtype)
                    out[places[i] + pair, r * 8 : (r + 1) * 8, at] = value

    def two_tiles(step, carry):
        one_tile(2 * step)
        one_tile(2 * step + 1)
        return carry

    lax.fori_loop(0, 2, two_tiles, 0)


def quarter_kernel(tab, first_x, second_x, out):
    project_rows(tab, first_x, second_x, out, (0, 2))


def last_kernel(tab, first_x, second_x, near_1, near_2, far_1, out):
    x, z_high = lax.axis_index("x"), lax.axis_index("z_hi")
    near_at, far_at = 8 * z_high, 8 * (1 - z_high)
    places = [2 * ((x + step) & 3) for step in range(4)]
    for step, part in ((0, near_1), (2, near_2)):
        for i in range(2):
            out[pl.ds(near_at + places[step + i], 2)] = part[2 * i : 2 * i + 2]
    for i in range(2):
        out[pl.ds(far_at + places[i], 2)] = far_1[2 * i : 2 * i + 2]
    project_rows(tab, first_x, second_x, out, (far_at + places[2], far_at + places[3]))


def project(kernel, owners, operands, name):
    return pl.pallas_call(
        kernel,
        out_shape=jax.ShapeDtypeStruct((owners, 16, 512), jnp.bfloat16),
        in_specs=[VMEM] * len(operands),
        out_specs=VMEM,
        compiler_params=pltpu.CompilerParams(vmem_limit_bytes=8 * 2**20),
        name=name,
    )(*operands)


def shards(sinogram, detector_coord):
    slices, angles, bins = sinogram.shape
    width = detector_coord.shape[2]
    core = lax.axis_index("core")
    swap = [(0, 1), (1, 0)]

    by_core = detector_coord.reshape(angles, 2, 2, 2, width)
    keep = lax.dynamic_index_in_dim(by_core, core, 2, keepdims=False).reshape(8, width)
    give = lax.dynamic_index_in_dim(by_core, 1 - core, 2, keepdims=False).reshape(8, width)
    own = jnp.stack([keep, lax.ppermute(give, "core", swap)])
    other = lax.ppermute(own, "z_hi", swap)

    def from_x(array, step):
        return lax.ppermute(array, "x", [((i + step) % 4, i) for i in range(4)])

    other_sino = lax.ppermute(sinogram, "core", swap)
    tab = filter_rows(
        sinogram.reshape(slices * angles, bins), other_sino.reshape(slices * angles, bins)
    )
    near = [own] + [from_x(own, s) for s in (1, 2, 3)]
    near_1 = project(quarter_kernel, 4, [tab, *near[:2]], "near_1")
    other, near_1 = lax.optimization_barrier((other, near_1))
    far = [other] + [from_x(other, s) for s in (1, 2, 3)]
    near_2 = project(quarter_kernel, 4, [tab, *near[2:]], "near_2")
    far_1 = project(quarter_kernel, 4, [tab, *far[:2]], "far_1")
    partial = project(last_kernel, 16, [tab, *far[2:], near_1, near_2, far_1], "far_2")
    parts = lax.all_to_all(partial, ("y", "z_lo"), 0, 0, tiled=True)
    scale = jnp.float32(math.pi / (angles * lax.axis_size(("y", "z_lo", "core"))))
    image_rows = jnp.sum(parts.astype(jnp.float32), axis=0) * scale
    return image_rows.reshape(2, slices, width)


def solution(mesh):
    names = ("y", "z_lo", "core", "z_hi", "x")
    fine = Mesh(mesh.devices.reshape(4, 4, 2, 2, 4), names)
    ang, sl = ("y", "z_lo", "core"), ("z_hi", "x")
    in_specs = (P(sl, ang, None), P(ang, sl, None))
    return jax.shard_map(
        shards, mesh=fine, in_specs=in_specs, out_specs=P(ang, sl, None), check_vma=False
    )
```

```python
import math

import jax
import jax.numpy as jnp
from jax import lax
from jax.experimental import pallas as pl
from jax.experimental.pallas import tpu as pltpu
from jax.sharding import Mesh
from jax.sharding import PartitionSpec as P

LANES = 128
LANE_DIMS = lax.GatherDimensionNumbers(
    offset_dims=(),
    collapsed_slice_dims=(1,),
    start_index_map=(1,),
    operand_batching_dims=(0,),
    start_indices_batching_dims=(0,),
)
VMEM = pl.BlockSpec(memory_space=pltpu.VMEM)


def lane_gather(table, lanes):
    return lax.gather(
        table, lanes[..., None], LANE_DIMS, (1, 1), mode=lax.GatherScatterMode.PROMISE_IN_BOUNDS
    )


def filter_kernel(own, other, out, strip):
    bins = own.shape[1]
    blocks = bins // LANES
    for j in range(2 * blocks - 1):
        first = lax.broadcasted_iota(jnp.int32, (LANES, LANES), 0)
        second = lax.broadcasted_iota(jnp.int32, (LANES, LANES), 1)
        offset = second - first + (j - blocks + 1) * LANES
        offset_sq = jnp.maximum((offset * offset).astype(jnp.float32), jnp.float32(1.0))
        values = jnp.where(
            (offset & 1) != 0, jnp.float32(-1.0 / math.pi**2) / offset_sq, jnp.float32(0.0)
        )
        if j == blocks - 1:
            values = jnp.where(offset == 0, jnp.float32(0.25), values)
        strip[:, j * LANES : (j + 1) * LANES] = values.astype(jnp.bfloat16)
    rows = jnp.concatenate([own[...], other[...]], axis=0)
    total = None
    for k in range(blocks):
        start = (blocks - 1 - k) * LANES
        part = jnp.dot(
            rows[:, k * LANES : (k + 1) * LANES],
            strip[:, start : start + bins],
            preferred_element_type=jnp.float32,
        )
        total = part if total is None else total + part
    out[...] = total.astype(jnp.bfloat16).astype(jnp.float32)


def filter_rows(own, other):
    rows, bins = own.shape
    return pl.pallas_call(
        filter_kernel,
        out_shape=jax.ShapeDtypeStruct((2 * rows, bins), jnp.float32),
        in_specs=[VMEM, VMEM],
        out_specs=VMEM,
        scratch_shapes=[pltpu.VMEM((LANES, 2 * bins - LANES), jnp.bfloat16)],
        compiler_params=pltpu.CompilerParams(vmem_limit_bytes=8 * 2**20),
        name="filter_rows",
    )(own, other)


def transposed(tiles):
    sublane = lax.broadcasted_iota(jnp.int32, (8, LANES), 0)
    for step in (4, 2, 1):
        low = (sublane & step) == 0
        done = list(tiles)
        for i in range(8):
            if not i & step:
                a, b = tiles[i], tiles[i + step]
                done[i] = jnp.where(low, a, pltpu.roll(b, step, 0))
                done[i + step] = jnp.where(low, pltpu.roll(a, 8 - step, 0), b)
        tiles = done
    return tiles


def project_rows(tab, first_x, second_x, out, places):
    sublane = lax.broadcasted_iota(jnp.int32, (8, LANES), 0)

    def one_tile(step):
        at = pl.ds(pl.multiple_of(step * LANES, LANES), LANES)
        sums = [None] * 8
        for core in range(2):
            first, second = first_x[core, :, at], second_x[core, :, at]
            for angle in range(2):
                if angle == 0:
                    c = jnp.where(sublane < 4, first, pltpu.roll(second, 4, 0))
                else:
                    c = jnp.where(sublane < 4, pltpu.roll(first, 4, 0), second)
                left = c >> 20
                fraction = (c & 1048575).astype(jnp.float32) * jnp.float32(1.0 / 1048576.0)
                w_left = (1.0 - fraction).astype(jnp.bfloat16).astype(jnp.float32)
                w_right = fraction.astype(jnp.bfloat16).astype(jnp.float32)
                bins = jnp.concatenate([left, left + 1], axis=0).astype(jnp.int16)
                lanes = bins & jnp.int16(LANES - 1)
                high = [(bins & jnp.int16(bit)) != 0 for bit in (128, 256, 512)]
                for s in range(8):
                    row = core * 16 + s * 2 + angle
                    taps = []
                    for k in range(8):
                        source = jnp.broadcast_to(
                            tab[row : row + 1, k * LANES : (k + 1) * LANES], (16, LANES)
                        )
                        taps.append(lane_gather(source.astype(jnp.bfloat16), lanes))
                    for mask in high:
                        taps = [
                            jnp.where(mask, taps[k + 1], taps[k]) for k in range(0, len(taps), 2)
                        ]
                    both = taps[0].astype(jnp.float32)
                    part = both[:8] * w_left + both[8:] * w_right
                    sums[s] = part if sums[s] is None else sums[s] + part
        rows = transposed(sums)
        for i in range(2):
            for pair in range(2):
                for r in range(2):
                    value = rows[i * 4 + pair * 2 + r].astype(out.dtype)
                    out[places[i] + pair, r * 8 : (r + 1) * 8, at] = value

    def two_tiles(step, carry):
        one_tile(2 * step)
        one_tile(2 * step + 1)
        return carry

    lax.fori_loop(0, 2, two_tiles, 0)


def quarter_kernel(tab, first_x, second_x, out):
    project_rows(tab, first_x, second_x, out, (0, 2))


def last_kernel(tab, first_x, second_x, near_1, near_2, far_1, out):
    x, z_high = lax.axis_index("x"), lax.axis_index("z_hi")
    near_at, far_at = 8 * z_high, 8 * (1 - z_high)
    places = [2 * ((x + step) & 3) for step in range(4)]
    for step, part in ((0, near_1), (2, near_2)):
        for i in range(2):
            out[pl.ds(near_at + places[step + i], 2)] = part[2 * i : 2 * i + 2]
    for i in range(2):
        out[pl.ds(far_at + places[i], 2)] = far_1[2 * i : 2 * i + 2]
    project_rows(tab, first_x, second_x, out, (far_at + places[2], far_at + places[3]))


def project(kernel, owners, operands):
    return pl.pallas_call(
        kernel,
        out_shape=jax.ShapeDtypeStruct((owners, 16, 512), jnp.bfloat16),
        in_specs=[VMEM] * len(operands),
        out_specs=VMEM,
        compiler_params=pltpu.CompilerParams(vmem_limit_bytes=8 * 2**20),
    )(*operands)


def permuted(array, axis, step, size):
    return lax.ppermute(array, axis, [((i + step) % size, i) for i in range(size)])


def image(sinogram, detector_coord):
    slices, angles, bins = sinogram.shape
    width = detector_coord.shape[2]
    core = lax.axis_index("core")

    by_core = detector_coord.reshape(angles, 2, 2, 2, width)
    keep = lax.dynamic_index_in_dim(by_core, core, 2, keepdims=False).reshape(8, width)
    give = lax.dynamic_index_in_dim(by_core, 1 - core, 2, keepdims=False).reshape(8, width)
    own = jnp.stack([keep, permuted(give, "core", 1, 2)])
    other = permuted(own, "z_hi", 1, 2)

    other_sino = permuted(sinogram, "core", 1, 2)
    tab = filter_rows(
        sinogram.reshape(slices * angles, bins), other_sino.reshape(slices * angles, bins)
    )
    near = [own] + [permuted(own, "x", s, 4) for s in (1, 2, 3)]
    near_1 = project(quarter_kernel, 4, [tab, *near[:2]])
    other, near_1 = lax.optimization_barrier((other, near_1))
    far = [other] + [permuted(other, "x", s, 4) for s in (1, 2, 3)]
    near_2 = project(quarter_kernel, 4, [tab, *near[2:]])
    far_1 = project(quarter_kernel, 4, [tab, *far[:2]])
    partial = project(last_kernel, 16, [tab, *far[2:], near_1, near_2, far_1])
    parts = lax.all_to_all(partial, ("y", "z_lo"), 0, 0, tiled=True)
    scale = jnp.float32(math.pi / (angles * lax.axis_size(("y", "z_lo", "core"))))
    image_rows = jnp.sum(parts.astype(jnp.float32), axis=0) * scale
    return image_rows.reshape(2, slices, width)


def solution(mesh):
    names = ("y", "z_lo", "core", "z_hi", "x")
    fine = Mesh(mesh.devices.reshape(4, 4, 2, 2, 4), names)
    ang, sl = ("y", "z_lo", "core"), ("z_hi", "x")
    in_specs = (P(sl, ang, None), P(ang, sl, None))
    return jax.shard_map(
        image, mesh=fine, in_specs=in_specs, out_specs=P(ang, sl, None), check_vma=False
    )
```

```python
import math

import jax
import jax.numpy as jnp
from jax import lax
from jax.experimental import pallas as pl
from jax.experimental.pallas import tpu as pltpu
from jax.sharding import Mesh
from jax.sharding import PartitionSpec as P

LANES = 128
LANE_DIMS = lax.GatherDimensionNumbers(
    offset_dims=(),
    collapsed_slice_dims=(1,),
    start_index_map=(1,),
    operand_batching_dims=(0,),
    start_indices_batching_dims=(0,),
)
VMEM = pl.BlockSpec(memory_space=pltpu.VMEM)


def lane_gather(table, lanes):
    return lax.gather(
        table, lanes[..., None], LANE_DIMS, (1, 1), mode=lax.GatherScatterMode.PROMISE_IN_BOUNDS
    )


def filter_kernel(own, other, out, strip):
    bins = own.shape[1]
    blocks = bins // LANES
    for j in range(2 * blocks - 1):
        first = lax.broadcasted_iota(jnp.int32, (LANES, LANES), 0)
        second = lax.broadcasted_iota(jnp.int32, (LANES, LANES), 1)
        offset = second - first + (j - blocks + 1) * LANES
        offset_sq = jnp.maximum((offset * offset).astype(jnp.float32), jnp.float32(1.0))
        values = jnp.where(
            (offset & 1) != 0, jnp.float32(-1.0 / math.pi**2) / offset_sq, jnp.float32(0.0)
        )
        if j == blocks - 1:
            values = jnp.where(offset == 0, jnp.float32(0.25), values)
        strip[:, j * LANES : (j + 1) * LANES] = values.astype(jnp.bfloat16)
    rows = jnp.concatenate([own[...], other[...]], axis=0)
    total = None
    for k in range(blocks):
        start = (blocks - 1 - k) * LANES
        part = jnp.dot(
            rows[:, k * LANES : (k + 1) * LANES],
            strip[:, start : start + bins],
            preferred_element_type=jnp.float32,
        )
        total = part if total is None else total + part
    out[...] = total.astype(jnp.bfloat16).astype(jnp.float32)


def filter_rows(own, other):
    rows, bins = own.shape
    return pl.pallas_call(
        filter_kernel,
        out_shape=jax.ShapeDtypeStruct((2 * rows, bins), jnp.float32),
        in_specs=[VMEM, VMEM],
        out_specs=VMEM,
        scratch_shapes=[pltpu.VMEM((LANES, 2 * bins - LANES), jnp.bfloat16)],
        compiler_params=pltpu.CompilerParams(vmem_limit_bytes=8 * 2**20),
        name="filter_rows",
    )(own, other)


def transposed(tiles):
    sublane = lax.broadcasted_iota(jnp.int32, (8, LANES), 0)
    for step in (4, 2, 1):
        low = (sublane & step) == 0
        done = list(tiles)
        for i in range(8):
            if not i & step:
                a, b = tiles[i], tiles[i + step]
                done[i] = jnp.where(low, a, pltpu.roll(b, step, 0))
                done[i + step] = jnp.where(low, pltpu.roll(a, 8 - step, 0), b)
        tiles = done
    return tiles


def packed(coords):
    tiles = [coords[..., p * LANES : (p + 1) * LANES] >> 6 for p in range(4)]
    words = [tiles[p] | ((tiles[3] >> (8 * p)) << 24) for p in range(3)]
    return jnp.concatenate(words, axis=-1)


def unpacked(words):
    tiles = [words[:, p * LANES : (p + 1) * LANES] for p in range(3)]
    top = [lax.shift_right_logical(tile, 24) for tile in tiles]
    return [tile & 16777215 for tile in tiles] + [top[0] | (top[1] << 8) | (top[2] << 16)]


def project_rows(tab, first_x, second_x, out, coords, places):
    sublane = lax.broadcasted_iota(jnp.int32, (8, LANES), 0)
    for core in range(2):
        tiles = zip(unpacked(first_x[core]), unpacked(second_x[core]))
        for p, (first, second) in enumerate(tiles):
            coords[p, 2 * core] = jnp.where(sublane < 4, first, pltpu.roll(second, 4, 0))
            coords[p, 2 * core + 1] = jnp.where(sublane < 4, pltpu.roll(first, 4, 0), second)

    def one_tile(step):
        at = pl.ds(pl.multiple_of(step * LANES, LANES), LANES)
        sums = [None] * 8
        for core in range(2):
            for angle in range(2):
                c = coords[step, 2 * core + angle]
                left = c >> 14
                fraction = (c & 16383).astype(jnp.float32) * jnp.float32(1.0 / 16384.0)
                w_left = (1.0 - fraction).astype(jnp.bfloat16).astype(jnp.float32)
                w_right = fraction.astype(jnp.bfloat16).astype(jnp.float32)
                bins = jnp.concatenate([left, left + 1], axis=0).astype(jnp.int16)
                lanes = bins & jnp.int16(LANES - 1)
                high = [(bins & jnp.int16(bit)) != 0 for bit in (128, 256, 512)]
                for s in range(8):
                    row = core * 16 + s * 2 + angle
                    taps = []
                    for k in range(8):
                        source = jnp.broadcast_to(
                            tab[row : row + 1, k * LANES : (k + 1) * LANES], (16, LANES)
                        )
                        taps.append(lane_gather(source.astype(jnp.bfloat16), lanes))
                    for mask in high:
                        taps = [
                            jnp.where(mask, taps[k + 1], taps[k]) for k in range(0, len(taps), 2)
                        ]
                    both = taps[0].astype(jnp.float32)
                    part = both[:8] * w_left + both[8:] * w_right
                    sums[s] = part if sums[s] is None else sums[s] + part
        rows = transposed(sums)
        for i in range(2):
            for pair in range(2):
                for r in range(2):
                    value = rows[i * 4 + pair * 2 + r].astype(out.dtype)
                    out[places[i] + pair, r * 8 : (r + 1) * 8, at] = value

    def two_tiles(step, carry):
        one_tile(2 * step)
        one_tile(2 * step + 1)
        return carry

    lax.fori_loop(0, 2, two_tiles, 0)


def quarter_kernel(tab, first_x, second_x, out, coords):
    project_rows(tab, first_x, second_x, out, coords, (0, 2))


def last_kernel(tab, first_x, second_x, near_1, near_2, far_1, out, coords):
    x, z_high = lax.axis_index("x"), lax.axis_index("z_hi")
    near_at, far_at = 8 * z_high, 8 * (1 - z_high)
    places = [2 * ((x + step) & 3) for step in range(4)]
    for base, part, steps in ((near_at, near_1, (0, 3)), (near_at, near_2, (2, 1)), (far_at, far_1, (0, 3))):
        for i in range(2):
            out[pl.ds(base + places[steps[i]], 2)] = part[2 * i : 2 * i + 2]
    project_rows(tab, first_x, second_x, out, coords, (far_at + places[2], far_at + places[1]))


def project(kernel, owners, operands):
    return pl.pallas_call(
        kernel,
        out_shape=jax.ShapeDtypeStruct((owners, 16, 512), jnp.bfloat16),
        in_specs=[VMEM] * len(operands),
        out_specs=VMEM,
        scratch_shapes=[pltpu.VMEM((4, 4, 8, LANES), jnp.int32)],
        compiler_params=pltpu.CompilerParams(vmem_limit_bytes=8 * 2**20),
    )(*operands)


def permuted(array, axis, step, size):
    return lax.ppermute(array, axis, [((i + step) % size, i) for i in range(size)])


def image(sinogram, detector_coord):
    slices, angles, bins = sinogram.shape
    width = detector_coord.shape[2]
    core = lax.axis_index("core")

    words = packed(detector_coord).reshape(angles, 2, 2, 2, 3 * LANES)
    keep = lax.dynamic_index_in_dim(words, core, 2, keepdims=False).reshape(8, 3 * LANES)
    give = lax.dynamic_index_in_dim(words, 1 - core, 2, keepdims=False).reshape(8, 3 * LANES)
    own = jnp.stack([keep, permuted(give, "core", 1, 2)])
    other = permuted(own, "z_hi", 1, 2)

    other_sino = permuted(sinogram, "core", 1, 2)
    tab = filter_rows(
        sinogram.reshape(slices * angles, bins), other_sino.reshape(slices * angles, bins)
    )
    near = [own] + [permuted(own, "x", s, 4) for s in (1, 2, 3)]
    near_1 = project(quarter_kernel, 4, [tab, near[0], near[3]])
    other, near_1 = lax.optimization_barrier((other, near_1))
    far = [other] + [permuted(other, "x", s, 4) for s in (1, 2, 3)]
    near_2 = project(quarter_kernel, 4, [tab, near[2], near[1]])
    far_1 = project(quarter_kernel, 4, [tab, far[0], far[3]])
    operands = [tab, far[2], far[1], near_1, near_2, far_1]
    partial = project(last_kernel, 16, operands)
    parts = lax.all_to_all(partial, ("y", "z_lo"), 0, 0, tiled=True)
    scale = jnp.float32(math.pi / (angles * lax.axis_size(("y", "z_lo", "core"))))
    image_rows = jnp.sum(parts.astype(jnp.float32), axis=0) * scale
    return image_rows.reshape(2, slices, width)


def solution(mesh):
    names = ("y", "z_lo", "core", "z_hi", "x")
    fine = Mesh(mesh.devices.reshape(4, 4, 2, 2, 4), names)
    ang, sl = ("y", "z_lo", "core"), ("z_hi", "x")
    in_specs = (P(sl, ang, None), P(ang, sl, None))
    return jax.shard_map(
        image, mesh=fine, in_specs=in_specs, out_specs=P(ang, sl, None), check_vma=False
    )
```

```python
import math

import jax
import jax.numpy as jnp
from jax import lax
from jax.experimental import pallas as pl
from jax.experimental.pallas import tpu as pltpu
from jax.sharding import Mesh
from jax.sharding import PartitionSpec as P

LANES = 128
LANE_DIMS = lax.GatherDimensionNumbers(
    offset_dims=(),
    collapsed_slice_dims=(1,),
    start_index_map=(1,),
    operand_batching_dims=(0,),
    start_indices_batching_dims=(0,),
)
VMEM = pl.BlockSpec(memory_space=pltpu.VMEM)


def lane_gather(table, lanes):
    return lax.gather(
        table, lanes[..., None], LANE_DIMS, (1, 1), mode=lax.GatherScatterMode.PROMISE_IN_BOUNDS
    )


def filter_kernel(own, other, out, strip):
    bins = own.shape[1]
    blocks = bins // LANES
    for j in range(2 * blocks - 1):
        first = lax.broadcasted_iota(jnp.int32, (LANES, LANES), 0)
        second = lax.broadcasted_iota(jnp.int32, (LANES, LANES), 1)
        offset = second - first + (j - blocks + 1) * LANES
        offset_sq = jnp.maximum((offset * offset).astype(jnp.float32), jnp.float32(1.0))
        values = jnp.where(
            (offset & 1) != 0, jnp.float32(-1.0 / math.pi**2) / offset_sq, jnp.float32(0.0)
        )
        if j == blocks - 1:
            values = jnp.where(offset == 0, jnp.float32(0.25), values)
        strip[:, j * LANES : (j + 1) * LANES] = values.astype(jnp.bfloat16)
    rows = jnp.concatenate([own[...], other[...]], axis=0)
    total = None
    for k in range(blocks):
        start = (blocks - 1 - k) * LANES
        part = jnp.dot(
            rows[:, k * LANES : (k + 1) * LANES],
            strip[:, start : start + bins],
            preferred_element_type=jnp.float32,
        )
        total = part if total is None else total + part
    out[...] = total.astype(jnp.bfloat16).astype(jnp.float32)


def filter_rows(own, other):
    rows, bins = own.shape
    return pl.pallas_call(
        filter_kernel,
        out_shape=jax.ShapeDtypeStruct((2 * rows, bins), jnp.float32),
        in_specs=[VMEM, VMEM],
        out_specs=VMEM,
        scratch_shapes=[pltpu.VMEM((LANES, 2 * bins - LANES), jnp.bfloat16)],
        compiler_params=pltpu.CompilerParams(vmem_limit_bytes=8 * 2**20),
        name="filter_rows",
    )(own, other)


def transposed(tiles):
    sublane = lax.broadcasted_iota(jnp.int32, (8, LANES), 0)
    for step in (4, 2, 1):
        low = (sublane & step) == 0
        done = list(tiles)
        for i in range(8):
            if not i & step:
                a, b = tiles[i], tiles[i + step]
                done[i] = jnp.where(low, a, pltpu.roll(b, step, 0))
                done[i + step] = jnp.where(low, pltpu.roll(a, 8 - step, 0), b)
        tiles = done
    return tiles


def packed(coords):
    tiles = [coords[..., p * LANES : (p + 1) * LANES] >> 6 for p in range(4)]
    words = [tiles[p] | ((tiles[3] >> (8 * p)) << 24) for p in range(3)]
    return jnp.concatenate(words, axis=-1)


def unpacked(words):
    tiles = [words[:, p * LANES : (p + 1) * LANES] for p in range(3)]
    top = [lax.shift_right_logical(tile, 24) for tile in tiles]
    return [tile & 16777215 for tile in tiles] + [top[0] | (top[1] << 8) | (top[2] << 16)]


def project_rows(tab, words, out, place):
    sublane = lax.broadcasted_iota(jnp.int32, (8, LANES), 0)
    tiles = [unpacked(words[core]) for core in range(2)]
    for p in range(4):
        sums = [None] * 8
        for core in range(2):
            c = tiles[core][p]
            left = c >> 14
            fraction = (c & 16383).astype(jnp.float32) * jnp.float32(1.0 / 16384.0)
            w_left = (1.0 - fraction).astype(jnp.bfloat16).astype(jnp.float32)
            w_right = fraction.astype(jnp.bfloat16).astype(jnp.float32)
            bins = jnp.concatenate([left, left + 1], axis=0).astype(jnp.int16)
            lanes = bins & jnp.int16(LANES - 1)
            high = [(bins & jnp.int16(bit)) != 0 for bit in (128, 256, 512)]
            for s in range(8):
                row = core * 16 + s * 2
                taps = []
                for k in range(8):
                    at = slice(k * LANES, (k + 1) * LANES)
                    source = jnp.where(
                        sublane < 4,
                        jnp.broadcast_to(tab[row : row + 1, at], (8, LANES)),
                        jnp.broadcast_to(tab[row + 1 : row + 2, at], (8, LANES)),
                    )
                    source = jnp.concatenate([source, source], axis=0).astype(jnp.bfloat16)
                    taps.append(lane_gather(source, lanes))
                for mask in high:
                    taps = [jnp.where(mask, taps[k + 1], taps[k]) for k in range(0, len(taps), 2)]
                both = taps[0].astype(jnp.float32)
                part = both[:8] * w_left + both[8:] * w_right
                sums[s] = part if sums[s] is None else sums[s] + part
        rows = transposed([total + pltpu.roll(total, 4, 0) for total in sums])
        for pair in range(2):
            for r in range(2):
                value = rows[pair * 2 + r].astype(out.dtype)
                out[place + pair, r * 8 : (r + 1) * 8, p * LANES : (p + 1) * LANES] = value


def array_kernel(tab, words, out):
    project_rows(tab, words, out, 0)


ORDER = ((0, 0), (0, 3), (0, 2), (0, 1), (1, 0), (1, 3), (1, 2), (1, 1))


def last_kernel(tab, words, *refs):
    parts, out = refs[:-1], refs[-1]
    x, z_high = lax.axis_index("x"), lax.axis_index("z_hi")
    places = [
        8 * (1 - z_high if far else z_high) + 2 * ((x + step) & 3) for far, step in ORDER
    ]
    for place, part in zip(places, parts):
        out[pl.ds(place, 2)] = part[...]
    project_rows(tab, words, out, places[-1])


def project(kernel, owners, operands):
    return pl.pallas_call(
        kernel,
        out_shape=jax.ShapeDtypeStruct((owners, 16, 512), jnp.bfloat16),
        in_specs=[VMEM] * len(operands),
        out_specs=VMEM,
        compiler_params=pltpu.CompilerParams(vmem_limit_bytes=8 * 2**20),
    )(*operands)


def permuted(array, axis, step, size):
    return lax.ppermute(array, axis, [((i + step) % size, i) for i in range(size)])


def image(sinogram, detector_coord):
    slices, angles, bins = sinogram.shape
    width = detector_coord.shape[2]
    core = lax.axis_index("core")

    words = packed(detector_coord).reshape(angles, 2, 2, 2, 3 * LANES)
    keep = lax.dynamic_index_in_dim(words, core, 2, keepdims=False).reshape(8, 3 * LANES)
    give = lax.dynamic_index_in_dim(words, 1 - core, 2, keepdims=False).reshape(8, 3 * LANES)
    own = jnp.stack([keep, permuted(give, "core", 1, 2)])
    other = permuted(own, "z_hi", 1, 2)

    other_sino = permuted(sinogram, "core", 1, 2)
    tab = filter_rows(
        sinogram.reshape(slices * angles, bins), other_sino.reshape(slices * angles, bins)
    )
    near = [own] + [permuted(own, "x", s, 4) for s in (1, 2, 3)]
    done = [project(array_kernel, 2, [tab, near[s]]) for s in (0, 3, 2)]
    other, *done = lax.optimization_barrier((other, *done))
    far = [other] + [permuted(other, "x", s, 4) for s in (1, 2, 3)]
    done.append(project(array_kernel, 2, [tab, near[1]]))
    done += [project(array_kernel, 2, [tab, far[s]]) for s in (0, 3, 2)]
    partial = project(last_kernel, 16, [tab, far[1], *done])
    parts = lax.all_to_all(partial, ("y", "z_lo"), 0, 0, tiled=True)
    scale = jnp.float32(math.pi / (angles * lax.axis_size(("y", "z_lo", "core"))))
    image_rows = jnp.sum(parts.astype(jnp.float32), axis=0) * scale
    return image_rows.reshape(2, slices, width)


def solution(mesh):
    names = ("y", "z_lo", "core", "z_hi", "x")
    fine = Mesh(mesh.devices.reshape(4, 4, 2, 2, 4), names)
    ang, sl = ("y", "z_lo", "core"), ("z_hi", "x")
    in_specs = (P(sl, ang, None), P(ang, sl, None))
    return jax.shard_map(
        image, mesh=fine, in_specs=in_specs, out_specs=P(ang, sl, None), check_vma=False
    )
```

```python
import math

import jax
import jax.numpy as jnp
from jax import lax
from jax.experimental import pallas as pl
from jax.experimental.pallas import tpu as pltpu
from jax.sharding import Mesh
from jax.sharding import PartitionSpec as P

LANES = 128
LANE_DIMS = lax.GatherDimensionNumbers(
    offset_dims=(),
    collapsed_slice_dims=(1,),
    start_index_map=(1,),
    operand_batching_dims=(0,),
    start_indices_batching_dims=(0,),
)
VMEM = pl.BlockSpec(memory_space=pltpu.VMEM)


def lane_gather(table, lanes):
    return lax.gather(
        table, lanes[..., None], LANE_DIMS, (1, 1), mode=lax.GatherScatterMode.PROMISE_IN_BOUNDS
    )


def filter_kernel(own, other, out, strip):
    bins = own.shape[1]
    blocks = bins // LANES
    for j in range(2 * blocks - 1):
        first = lax.broadcasted_iota(jnp.int32, (LANES, LANES), 0)
        second = lax.broadcasted_iota(jnp.int32, (LANES, LANES), 1)
        offset = second - first + (j - blocks + 1) * LANES
        offset_sq = jnp.maximum((offset * offset).astype(jnp.float32), jnp.float32(1.0))
        values = jnp.where(
            (offset & 1) != 0, jnp.float32(-1.0 / math.pi**2) / offset_sq, jnp.float32(0.0)
        )
        if j == blocks - 1:
            values = jnp.where(offset == 0, jnp.float32(0.25), values)
        strip[:, j * LANES : (j + 1) * LANES] = values.astype(jnp.bfloat16)
    rows = jnp.concatenate([own[...], other[...]], axis=0)
    total = None
    for k in range(blocks):
        start = (blocks - 1 - k) * LANES
        part = jnp.dot(
            rows[:, k * LANES : (k + 1) * LANES],
            strip[:, start : start + bins],
            preferred_element_type=jnp.float32,
        )
        total = part if total is None else total + part
    out[...] = total.astype(jnp.bfloat16).astype(jnp.float32)


def filter_rows(own, other):
    rows, bins = own.shape
    return pl.pallas_call(
        filter_kernel,
        out_shape=jax.ShapeDtypeStruct((2 * rows, bins), jnp.float32),
        in_specs=[VMEM, VMEM],
        out_specs=VMEM,
        scratch_shapes=[pltpu.VMEM((LANES, 2 * bins - LANES), jnp.bfloat16)],
        compiler_params=pltpu.CompilerParams(vmem_limit_bytes=8 * 2**20),
        name="filter_rows",
    )(own, other)


def transposed(tiles):
    sublane = lax.broadcasted_iota(jnp.int32, (8, LANES), 0)
    for step in (4, 2, 1):
        low = (sublane & step) == 0
        done = list(tiles)
        for i in range(8):
            if not i & step:
                a, b = tiles[i], tiles[i + step]
                done[i] = jnp.where(low, a, pltpu.roll(b, step, 0))
                done[i + step] = jnp.where(low, pltpu.roll(a, 8 - step, 0), b)
        tiles = done
    return tiles


def packed(coords):
    tiles = [coords[..., p * LANES : (p + 1) * LANES] >> 6 for p in range(4)]
    words = [tiles[p] | ((tiles[3] >> (8 * p)) << 24) for p in range(3)]
    return jnp.concatenate(words, axis=-1)


def unpacked(words):
    tiles = [words[:, p * LANES : (p + 1) * LANES] for p in range(3)]
    top = [lax.shift_right_logical(tile, 24) for tile in tiles]
    return [tile & 16777215 for tile in tiles] + [top[0] | (top[1] << 8) | (top[2] << 16)]


def project_rows(tab, words, out, place):
    sublane = lax.broadcasted_iota(jnp.int32, (8, LANES), 0)
    tiles = [unpacked(words[core]) for core in range(2)]
    for p in range(4):
        sums = [None] * 8
        for core in range(2):
            c = tiles[core][p]
            left = c >> 14
            fraction = (c & 16383).astype(jnp.float32) * jnp.float32(1.0 / 16384.0)
            w_left = (1.0 - fraction).astype(jnp.bfloat16).astype(jnp.float32)
            w_right = fraction.astype(jnp.bfloat16).astype(jnp.float32)
            bins = jnp.concatenate([left, left + 1], axis=0).astype(jnp.int16)
            lanes = bins & jnp.int16(LANES - 1)
            high = [(bins & jnp.int16(bit)) != 0 for bit in (128, 256, 512)]
            for s in range(8):
                row = core * 16 + s * 2
                taps = []
                for k in range(8):
                    at = slice(k * LANES, (k + 1) * LANES)
                    source = jnp.where(
                        sublane < 4,
                        jnp.broadcast_to(tab[row : row + 1, at], (8, LANES)),
                        jnp.broadcast_to(tab[row + 1 : row + 2, at], (8, LANES)),
                    )
                    source = jnp.concatenate([source, source], axis=0).astype(jnp.bfloat16)
                    taps.append(lane_gather(source, lanes))
                for mask in high:
                    taps = [jnp.where(mask, taps[k + 1], taps[k]) for k in range(0, len(taps), 2)]
                both = taps[0].astype(jnp.float32)
                part = both[:8] * w_left + both[8:] * w_right
                sums[s] = part if sums[s] is None else sums[s] + part
        rows = transposed([total + pltpu.roll(total, 4, 0) for total in sums])
        for pair in range(2):
            for r in range(2):
                value = rows[pair * 2 + r].astype(out.dtype)
                out[place + pair, r * 8 : (r + 1) * 8, p * LANES : (p + 1) * LANES] = value


def array_kernel(tab, words, out):
    project_rows(tab, words, out, 0)


ORDER = ((0, 0), (0, 3), (0, 2), (0, 1), (1, 0), (1, 3), (1, 2), (1, 1))


def last_kernel(tab, words, *refs):
    parts, out = refs[:-1], refs[-1]
    x, z_high = lax.axis_index("x"), lax.axis_index("z_hi")
    places = [
        8 * (1 - z_high if far else z_high) + 2 * ((x + step) & 3) for far, step in ORDER
    ]
    for place, part in zip(places, parts):
        out[pl.ds(place, 2)] = part[...]
    project_rows(tab, words, out, places[-1])


def project(kernel, owners, operands):
    return pl.pallas_call(
        kernel,
        out_shape=jax.ShapeDtypeStruct((owners, 16, 512), jnp.bfloat16),
        in_specs=[VMEM] * len(operands),
        out_specs=VMEM,
        compiler_params=pltpu.CompilerParams(vmem_limit_bytes=8 * 2**20),
    )(*operands)


def permuted(array, axis, step, size):
    return lax.ppermute(array, axis, [((i + step) % size, i) for i in range(size)])


def image(sinogram, detector_coord):
    slices, angles, bins = sinogram.shape
    width = detector_coord.shape[2]
    core = lax.axis_index("core")

    words = packed(detector_coord).reshape(angles, 2, 2, 2, 3 * LANES)
    keep = lax.dynamic_index_in_dim(words, core, 2, keepdims=False).reshape(8, 3 * LANES)
    give = lax.dynamic_index_in_dim(words, 1 - core, 2, keepdims=False).reshape(8, 3 * LANES)
    own = jnp.stack([keep, permuted(give, "core", 1, 2)])
    other = permuted(own, "z_hi", 1, 2)

    other_sino = permuted(sinogram, "core", 1, 2)
    tab = filter_rows(
        sinogram.reshape(slices * angles, bins), other_sino.reshape(slices * angles, bins)
    )
    near = [own] + [permuted(own, "x", s, 4) for s in (1, 2, 3)]
    done = [project(array_kernel, 2, [tab, near[0]])]
    other, done[0] = lax.optimization_barrier((other, done[0]))
    far = [other] + [permuted(other, "x", s, 4) for s in (1, 2, 3)]
    done += [project(array_kernel, 2, [tab, near[s]]) for s in (3, 2, 1)]
    done += [project(array_kernel, 2, [tab, far[s]]) for s in (0, 3, 2)]
    partial = project(last_kernel, 16, [tab, far[1], *done])
    parts = lax.all_to_all(partial, ("y", "z_lo"), 0, 0, tiled=True)
    scale = jnp.float32(math.pi / (angles * lax.axis_size(("y", "z_lo", "core"))))
    image_rows = jnp.sum(parts.astype(jnp.float32), axis=0) * scale
    return image_rows.reshape(2, slices, width)


def solution(mesh):
    names = ("y", "z_lo", "core", "z_hi", "x")
    fine = Mesh(mesh.devices.reshape(4, 4, 2, 2, 4), names)
    ang, sl = ("y", "z_lo", "core"), ("z_hi", "x")
    in_specs = (P(sl, ang, None), P(ang, sl, None))
    return jax.shard_map(
        image, mesh=fine, in_specs=in_specs, out_specs=P(ang, sl, None), check_vma=False
    )
```

```python
import math

import jax
import jax.numpy as jnp
from jax import lax
from jax.experimental import pallas as pl
from jax.experimental.pallas import tpu as pltpu
from jax.sharding import Mesh
from jax.sharding import PartitionSpec as P

LANES = 128
LANE_DIMS = lax.GatherDimensionNumbers(
    offset_dims=(),
    collapsed_slice_dims=(1,),
    start_index_map=(1,),
    operand_batching_dims=(0,),
    start_indices_batching_dims=(0,),
)
VMEM = pl.BlockSpec(memory_space=pltpu.VMEM)


def lane_gather(table, lanes):
    return lax.gather(
        table, lanes[..., None], LANE_DIMS, (1, 1), mode=lax.GatherScatterMode.PROMISE_IN_BOUNDS
    )


def filter_kernel(own, other, out, strip):
    bins = own.shape[1]
    blocks = bins // LANES
    for j in range(2 * blocks - 1):
        first = lax.broadcasted_iota(jnp.int32, (LANES, LANES), 0)
        second = lax.broadcasted_iota(jnp.int32, (LANES, LANES), 1)
        offset = second - first + (j - blocks + 1) * LANES
        offset_sq = jnp.maximum((offset * offset).astype(jnp.float32), jnp.float32(1.0))
        values = jnp.where(
            (offset & 1) != 0, jnp.float32(-1.0 / math.pi**2) / offset_sq, jnp.float32(0.0)
        )
        if j == blocks - 1:
            values = jnp.where(offset == 0, jnp.float32(0.25), values)
        strip[:, j * LANES : (j + 1) * LANES] = values.astype(jnp.bfloat16)
    rows = jnp.concatenate([own[...], other[...]], axis=0)
    total = None
    for k in range(blocks):
        start = (blocks - 1 - k) * LANES
        part = jnp.dot(
            rows[:, k * LANES : (k + 1) * LANES],
            strip[:, start : start + bins],
            preferred_element_type=jnp.float32,
        )
        total = part if total is None else total + part
    out[...] = total.astype(jnp.bfloat16).astype(jnp.float32)


def transposed(tiles):
    sublane = lax.broadcasted_iota(jnp.int32, (8, LANES), 0)
    for step in (4, 2, 1):
        low = (sublane & step) == 0
        done = list(tiles)
        for i in range(8):
            if not i & step:
                a, b = tiles[i], tiles[i + step]
                done[i] = jnp.where(low, a, pltpu.roll(b, step, 0))
                done[i + step] = jnp.where(low, pltpu.roll(a, 8 - step, 0), b)
        tiles = done
    return tiles


def packed(coords):
    tiles = [coords[..., p * LANES : (p + 1) * LANES] >> 6 for p in range(4)]
    words = [tiles[p] | ((tiles[3] >> (8 * p)) << 24) for p in range(3)]
    return jnp.concatenate(words, axis=-1)


def unpacked(words):
    tiles = [words[:, p * LANES : (p + 1) * LANES] for p in range(3)]
    top = [lax.shift_right_logical(tile, 24) for tile in tiles]
    return [tile & 16777215 for tile in tiles] + [top[0] | (top[1] << 8) | (top[2] << 16)]


def project_rows(tab, words, out, place):
    sublane = lax.broadcasted_iota(jnp.int32, (8, LANES), 0)
    tiles = [unpacked(words[core]) for core in range(2)]
    for p in range(4):
        sums = [None] * 8
        for core in range(2):
            c = tiles[core][p]
            left = c >> 14
            fraction = (c & 16383).astype(jnp.float32) * jnp.float32(1.0 / 16384.0)
            w_left = (1.0 - fraction).astype(jnp.bfloat16).astype(jnp.float32)
            w_right = fraction.astype(jnp.bfloat16).astype(jnp.float32)
            bins = jnp.concatenate([left, left + 1], axis=0).astype(jnp.int16)
            lanes = bins & jnp.int16(LANES - 1)
            high = [(bins & jnp.int16(bit)) != 0 for bit in (128, 256, 512)]
            for s in range(8):
                row = core * 16 + s * 2
                taps = []
                for k in range(8):
                    at = slice(k * LANES, (k + 1) * LANES)
                    source = jnp.where(
                        sublane < 4,
                        jnp.broadcast_to(tab[row : row + 1, at], (8, LANES)),
                        jnp.broadcast_to(tab[row + 1 : row + 2, at], (8, LANES)),
                    )
                    source = jnp.concatenate([source, source], axis=0).astype(jnp.bfloat16)
                    taps.append(lane_gather(source, lanes))
                for mask in high:
                    taps = [jnp.where(mask, taps[k + 1], taps[k]) for k in range(0, len(taps), 2)]
                both = taps[0].astype(jnp.float32)
                part = both[:8] * w_left + both[8:] * w_right
                sums[s] = part if sums[s] is None else sums[s] + part
        rows = transposed([total + pltpu.roll(total, 4, 0) for total in sums])
        for pair in range(2):
            for r in range(2):
                value = rows[pair * 2 + r].astype(out.dtype)
                out[place + pair, r * 8 : (r + 1) * 8, p * LANES : (p + 1) * LANES] = value


def prepare(own, other, words, tab, near, strip):
    filter_kernel(own, other, tab, strip)
    project_rows(tab, words, near, 0)


def early_kernel(own, other, words, tab, near, strip):
    @pl.when(lax.axis_index("z_hi") == 0)
    def _():
        prepare(own, other, words, tab, near, strip)


def late_kernel(own, other, words, tab_early, near_early, tab, near, strip):
    early = lax.axis_index("z_hi") == 0

    @pl.when(early)
    def _():
        tab[...] = tab_early[...]
        near[...] = near_early[...]

    @pl.when(jnp.logical_not(early))
    def _():
        prepare(own, other, words, tab, near, strip)


def prepared(kernel, operands):
    rows, bins = operands[0].shape
    return pl.pallas_call(
        kernel,
        out_shape=(
            jax.ShapeDtypeStruct((2 * rows, bins), jnp.float32),
            jax.ShapeDtypeStruct((2, 16, 512), jnp.bfloat16),
        ),
        in_specs=[VMEM] * len(operands),
        out_specs=(VMEM, VMEM),
        scratch_shapes=[pltpu.VMEM((LANES, 2 * bins - LANES), jnp.bfloat16)],
        compiler_params=pltpu.CompilerParams(vmem_limit_bytes=8 * 2**20),
    )(*operands)


def array_kernel(tab, words, out):
    project_rows(tab, words, out, 0)


ORDER = ((0, 0), (0, 3), (0, 2), (0, 1), (1, 0), (1, 3), (1, 2), (1, 1))


def last_kernel(tab, words, *refs):
    parts, out = refs[:-1], refs[-1]
    x, z_high = lax.axis_index("x"), lax.axis_index("z_hi")
    places = [
        8 * (1 - z_high if far else z_high) + 2 * ((x + step) & 3) for far, step in ORDER
    ]
    for place, part in zip(places, parts):
        out[pl.ds(place, 2)] = part[...]
    project_rows(tab, words, out, places[-1])


def project(kernel, owners, operands):
    return pl.pallas_call(
        kernel,
        out_shape=jax.ShapeDtypeStruct((owners, 16, 512), jnp.bfloat16),
        in_specs=[VMEM] * len(operands),
        out_specs=VMEM,
        compiler_params=pltpu.CompilerParams(vmem_limit_bytes=8 * 2**20),
    )(*operands)


def permuted(array, axis, step, size):
    return lax.ppermute(array, axis, [((i + step) % size, i) for i in range(size)])


def image(sinogram, detector_coord):
    slices, angles, bins = sinogram.shape
    width = detector_coord.shape[2]
    core = lax.axis_index("core")

    words = packed(detector_coord).reshape(angles, 2, 2, 2, 3 * LANES)
    keep = lax.dynamic_index_in_dim(words, core, 2, keepdims=False).reshape(8, 3 * LANES)
    give = lax.dynamic_index_in_dim(words, 1 - core, 2, keepdims=False).reshape(8, 3 * LANES)
    own = jnp.stack([keep, permuted(give, "core", 1, 2)])
    other = permuted(own, "z_hi", 1, 2)

    sinos = [sinogram, permuted(sinogram, "core", 1, 2)]
    operands = [sino.reshape(slices * angles, bins) for sino in sinos] + [own]
    early = prepared(early_kernel, operands)
    tab, near_0 = prepared(late_kernel, [*operands, *early])
    near = [own] + [permuted(own, "x", s, 4) for s in (1, 2, 3)]
    other, near_0 = lax.optimization_barrier((other, near_0))
    far = [other] + [permuted(other, "x", s, 4) for s in (1, 2, 3)]
    done = [near_0]
    done += [project(array_kernel, 2, [tab, near[s]]) for s in (3, 2, 1)]
    done += [project(array_kernel, 2, [tab, far[s]]) for s in (0, 3, 2)]
    partial = project(last_kernel, 16, [tab, far[1], *done])
    parts = lax.all_to_all(partial, ("y", "z_lo"), 0, 0, tiled=True)
    scale = jnp.float32(math.pi / (angles * lax.axis_size(("y", "z_lo", "core"))))
    image_rows = jnp.sum(parts.astype(jnp.float32), axis=0) * scale
    return image_rows.reshape(2, slices, width)


def solution(mesh):
    names = ("y", "z_lo", "core", "z_hi", "x")
    fine = Mesh(mesh.devices.reshape(4, 4, 2, 2, 4), names)
    ang, sl = ("y", "z_lo", "core"), ("z_hi", "x")
    in_specs = (P(sl, ang, None), P(ang, sl, None))
    return jax.shard_map(
        image, mesh=fine, in_specs=in_specs, out_specs=P(ang, sl, None), check_vma=False
    )
```

```python
import math

import jax
import jax.numpy as jnp
from jax import lax
from jax.experimental import pallas as pl
from jax.experimental.pallas import tpu as pltpu
from jax.sharding import Mesh
from jax.sharding import PartitionSpec as P

LANES = 128
LANE_DIMS = lax.GatherDimensionNumbers(
    offset_dims=(),
    collapsed_slice_dims=(1,),
    start_index_map=(1,),
    operand_batching_dims=(0,),
    start_indices_batching_dims=(0,),
)
VMEM = pl.BlockSpec(memory_space=pltpu.VMEM)


def lane_gather(table, lanes):
    return lax.gather(
        table, lanes[..., None], LANE_DIMS, (1, 1), mode=lax.GatherScatterMode.PROMISE_IN_BOUNDS
    )


def filter_kernel(own, other, out, strip):
    bins = own.shape[1]
    blocks = bins // LANES
    for j in range(2 * blocks - 1):
        first = lax.broadcasted_iota(jnp.int32, (LANES, LANES), 0)
        second = lax.broadcasted_iota(jnp.int32, (LANES, LANES), 1)
        offset = second - first + (j - blocks + 1) * LANES
        offset_sq = jnp.maximum((offset * offset).astype(jnp.float32), jnp.float32(1.0))
        values = jnp.where(
            (offset & 1) != 0, jnp.float32(-1.0 / math.pi**2) / offset_sq, jnp.float32(0.0)
        )
        if j == blocks - 1:
            values = jnp.where(offset == 0, jnp.float32(0.25), values)
        strip[:, j * LANES : (j + 1) * LANES] = values.astype(jnp.bfloat16)
    rows = jnp.concatenate([own[...], other[...]], axis=0)
    total = None
    for k in range(blocks):
        start = (blocks - 1 - k) * LANES
        part = jnp.dot(
            rows[:, k * LANES : (k + 1) * LANES],
            strip[:, start : start + bins],
            preferred_element_type=jnp.float32,
        )
        total = part if total is None else total + part
    out[...] = total.astype(jnp.bfloat16).astype(jnp.float32)


def filter_rows(own, other):
    rows, bins = own.shape
    return pl.pallas_call(
        filter_kernel,
        out_shape=jax.ShapeDtypeStruct((2 * rows, bins), jnp.float32),
        in_specs=[VMEM, VMEM],
        out_specs=VMEM,
        scratch_shapes=[pltpu.VMEM((LANES, 2 * bins - LANES), jnp.bfloat16)],
        compiler_params=pltpu.CompilerParams(vmem_limit_bytes=8 * 2**20),
        name="filter_rows",
    )(own, other)


def transposed(tiles):
    sublane = lax.broadcasted_iota(jnp.int32, (8, LANES), 0)
    for step in (4, 2, 1):
        low = (sublane & step) == 0
        done = list(tiles)
        for i in range(8):
            if not i & step:
                a, b = tiles[i], tiles[i + step]
                done[i] = jnp.where(low, a, pltpu.roll(b, step, 0))
                done[i + step] = jnp.where(low, pltpu.roll(a, 8 - step, 0), b)
        tiles = done
    return tiles


def packed(coords):
    tiles = [coords[..., p * LANES : (p + 1) * LANES] >> 6 for p in range(4)]
    words = [tiles[p] | ((tiles[3] >> (8 * p)) << 24) for p in range(3)]
    return jnp.concatenate(words, axis=-1)


def unpacked(words):
    tiles = [words[:, p * LANES : (p + 1) * LANES] for p in range(3)]
    top = [lax.shift_right_logical(tile, 24) for tile in tiles]
    return [tile & 16777215 for tile in tiles] + [top[0] | (top[1] << 8) | (top[2] << 16)]


def project_rows(tab, words, out, place):
    sublane = lax.broadcasted_iota(jnp.int32, (8, LANES), 0)
    tiles = [unpacked(words[core]) for core in range(2)]
    for p in range(4):
        sums = [None] * 8
        for core in range(2):
            c = tiles[core][p]
            left = c >> 14
            fraction = (c & 16383).astype(jnp.float32) * jnp.float32(1.0 / 16384.0)
            w_left = (1.0 - fraction).astype(jnp.bfloat16).astype(jnp.float32)
            w_right = fraction.astype(jnp.bfloat16).astype(jnp.float32)
            bins = jnp.concatenate([left, left + 1], axis=0).astype(jnp.int16)
            lanes = bins & jnp.int16(LANES - 1)
            high = [(bins & jnp.int16(bit)) != 0 for bit in (128, 256, 512)]
            for s in range(8):
                row = core * 16 + s * 2
                taps = []
                for k in range(8):
                    at = slice(k * LANES, (k + 1) * LANES)
                    source = jnp.where(
                        sublane < 4,
                        jnp.broadcast_to(tab[row : row + 1, at], (8, LANES)),
                        jnp.broadcast_to(tab[row + 1 : row + 2, at], (8, LANES)),
                    )
                    source = jnp.concatenate([source, source], axis=0).astype(jnp.bfloat16)
                    taps.append(lane_gather(source, lanes))
                for mask in high:
                    taps = [jnp.where(mask, taps[k + 1], taps[k]) for k in range(0, len(taps), 2)]
                both = taps[0].astype(jnp.float32)
                part = both[:8] * w_left + both[8:] * w_right
                sums[s] = part if sums[s] is None else sums[s] + part
        rows = transposed([total + pltpu.roll(total, 4, 0) for total in sums])
        for pair in range(2):
            for r in range(2):
                value = rows[pair * 2 + r].astype(out.dtype)
                out[place + pair, r * 8 : (r + 1) * 8, p * LANES : (p + 1) * LANES] = value


def array_kernel(tab, words, out):
    project_rows(tab, words, out, 0)


ORDER = ((0, 0), (0, 3), (0, 1), (1, 0), (1, 3), (1, 2), (1, 1), (0, 2))


def last_kernel(tab, words, *refs):
    parts, out = refs[:-1], refs[-1]
    x, z_high = lax.axis_index("x"), lax.axis_index("z_hi")
    places = [
        8 * (1 - z_high if far else z_high) + 2 * ((x + step) & 3) for far, step in ORDER
    ]
    for place, part in zip(places, parts):
        out[pl.ds(place, 2)] = part[...]
    project_rows(tab, words, out, places[-1])


def project(kernel, owners, operands):
    return pl.pallas_call(
        kernel,
        out_shape=jax.ShapeDtypeStruct((owners, 16, 512), jnp.bfloat16),
        in_specs=[VMEM] * len(operands),
        out_specs=VMEM,
        compiler_params=pltpu.CompilerParams(vmem_limit_bytes=8 * 2**20),
    )(*operands)


def permuted(array, axis, step, size):
    return lax.ppermute(array, axis, [((i + step) % size, i) for i in range(size)])


def image(sinogram, detector_coord):
    slices, angles, bins = sinogram.shape
    width = detector_coord.shape[2]
    core = lax.axis_index("core")

    words = packed(detector_coord).reshape(angles, 2, 2, 2, 3 * LANES)
    keep = lax.dynamic_index_in_dim(words, core, 2, keepdims=False).reshape(8, 3 * LANES)
    give = lax.dynamic_index_in_dim(words, 1 - core, 2, keepdims=False).reshape(8, 3 * LANES)
    own = jnp.stack([keep, permuted(give, "core", 1, 2)])
    other = permuted(own, "z_hi", 1, 2)

    other_sino = permuted(sinogram, "core", 1, 2)
    tab = filter_rows(
        sinogram.reshape(slices * angles, bins), other_sino.reshape(slices * angles, bins)
    )
    near = [own] + [permuted(own, "x", s, 4) for s in (1, 2, 3)]
    done = [project(array_kernel, 2, [tab, near[0]])]
    other, done[0] = lax.optimization_barrier((other, done[0]))
    far = [other] + [permuted(other, "x", s, 4) for s in (1, 2, 3)]
    done += [project(array_kernel, 2, [tab, near[s]]) for s in (3, 1)]
    done += [project(array_kernel, 2, [tab, far[s]]) for s in (0, 3, 2, 1)]
    partial = project(last_kernel, 16, [tab, near[2], *done])
    parts = lax.all_to_all(partial, ("y", "z_lo"), 0, 0, tiled=True)
    scale = jnp.float32(math.pi / (angles * lax.axis_size(("y", "z_lo", "core"))))
    image_rows = jnp.sum(parts.astype(jnp.float32), axis=0) * scale
    return image_rows.reshape(2, slices, width)


def solution(mesh):
    names = ("y", "z_lo", "core", "z_hi", "x")
    fine = Mesh(mesh.devices.reshape(4, 4, 2, 2, 4), names)
    ang, sl = ("y", "z_lo", "core"), ("z_hi", "x")
    in_specs = (P(sl, ang, None), P(ang, sl, None))
    return jax.shard_map(
        image, mesh=fine, in_specs=in_specs, out_specs=P(ang, sl, None), check_vma=False
    )
```

```python
import math

import jax
import jax.numpy as jnp
from jax import lax
from jax.experimental import pallas as pl
from jax.experimental.pallas import tpu as pltpu
from jax.sharding import Mesh
from jax.sharding import PartitionSpec as P

LANES = 128
LANE_DIMS = lax.GatherDimensionNumbers(
    offset_dims=(),
    collapsed_slice_dims=(1,),
    start_index_map=(1,),
    operand_batching_dims=(0,),
    start_indices_batching_dims=(0,),
)
VMEM = pl.BlockSpec(memory_space=pltpu.VMEM)


def lane_gather(table, lanes):
    return lax.gather(
        table, lanes[..., None], LANE_DIMS, (1, 1), mode=lax.GatherScatterMode.PROMISE_IN_BOUNDS
    )


def filter_kernel(own, other, out, strip):
    bins = own.shape[1]
    blocks = bins // LANES
    for j in range(2 * blocks - 1):
        first = lax.broadcasted_iota(jnp.int32, (LANES, LANES), 0)
        second = lax.broadcasted_iota(jnp.int32, (LANES, LANES), 1)
        offset = second - first + (j - blocks + 1) * LANES
        offset_sq = jnp.maximum((offset * offset).astype(jnp.float32), jnp.float32(1.0))
        values = jnp.where(
            (offset & 1) != 0, jnp.float32(-1.0 / math.pi**2) / offset_sq, jnp.float32(0.0)
        )
        if j == blocks - 1:
            values = jnp.where(offset == 0, jnp.float32(0.25), values)
        strip[:, j * LANES : (j + 1) * LANES] = values.astype(jnp.bfloat16)
    rows = jnp.concatenate([own[...], other[...]], axis=0)
    total = None
    for k in range(blocks):
        start = (blocks - 1 - k) * LANES
        part = jnp.dot(
            rows[:, k * LANES : (k + 1) * LANES],
            strip[:, start : start + bins],
            preferred_element_type=jnp.float32,
        )
        total = part if total is None else total + part
    out[...] = total.astype(jnp.bfloat16).astype(jnp.float32)


def transposed(tiles):
    sublane = lax.broadcasted_iota(jnp.int32, (8, LANES), 0)
    for step in (4, 2, 1):
        low = (sublane & step) == 0
        done = list(tiles)
        for i in range(8):
            if not i & step:
                a, b = tiles[i], tiles[i + step]
                done[i] = jnp.where(low, a, pltpu.roll(b, step, 0))
                done[i + step] = jnp.where(low, pltpu.roll(a, 8 - step, 0), b)
        tiles = done
    return tiles


def packed(coords):
    tiles = [coords[..., p * LANES : (p + 1) * LANES] >> 6 for p in range(4)]
    words = [tiles[p] | ((tiles[3] >> (8 * p)) << 24) for p in range(3)]
    return jnp.concatenate(words, axis=-1)


def unpacked(words):
    tiles = [words[:, p * LANES : (p + 1) * LANES] for p in range(3)]
    top = [lax.shift_right_logical(tile, 24) for tile in tiles]
    return [tile & 16777215 for tile in tiles] + [top[0] | (top[1] << 8) | (top[2] << 16)]


def project_rows(tab, words, out, place):
    sublane = lax.broadcasted_iota(jnp.int32, (8, LANES), 0)
    tiles = [unpacked(words[core]) for core in range(2)]
    for p in range(4):
        sums = [None] * 8
        for core in range(2):
            c = tiles[core][p]
            left = c >> 14
            fraction = (c & 16383).astype(jnp.float32) * jnp.float32(1.0 / 16384.0)
            w_left = (1.0 - fraction).astype(jnp.bfloat16).astype(jnp.float32)
            w_right = fraction.astype(jnp.bfloat16).astype(jnp.float32)
            bins = jnp.concatenate([left, left + 1], axis=0).astype(jnp.int16)
            lanes = bins & jnp.int16(LANES - 1)
            high = [(bins & jnp.int16(bit)) != 0 for bit in (128, 256, 512)]
            for s in range(8):
                row = core * 16 + s * 2
                taps = []
                for k in range(8):
                    at = slice(k * LANES, (k + 1) * LANES)
                    source = jnp.where(
                        sublane < 4,
                        jnp.broadcast_to(tab[row : row + 1, at], (8, LANES)),
                        jnp.broadcast_to(tab[row + 1 : row + 2, at], (8, LANES)),
                    )
                    source = jnp.concatenate([source, source], axis=0).astype(jnp.bfloat16)
                    taps.append(lane_gather(source, lanes))
                for mask in high:
                    taps = [jnp.where(mask, taps[k + 1], taps[k]) for k in range(0, len(taps), 2)]
                both = taps[0].astype(jnp.float32)
                part = both[:8] * w_left + both[8:] * w_right
                sums[s] = part if sums[s] is None else sums[s] + part
        rows = transposed([total + pltpu.roll(total, 4, 0) for total in sums])
        for pair in range(2):
            for r in range(2):
                value = rows[pair * 2 + r].astype(out.dtype)
                out[place + pair, r * 8 : (r + 1) * 8, p * LANES : (p + 1) * LANES] = value


def early_kernel(own, other, tab, strip):
    @pl.when(lax.axis_index("z_hi") == 0)
    def _():
        filter_kernel(own, other, tab, strip)


def late_kernel(own, other, words, tab_early, tab, near, strip):
    early = lax.axis_index("z_hi") == 0

    @pl.when(early)
    def _():
        tab[...] = tab_early[...]

    @pl.when(jnp.logical_not(early))
    def _():
        filter_kernel(own, other, tab, strip)

    project_rows(tab, words, near, 0)


def prepared(kernel, outs, operands):
    rows, bins = operands[0].shape
    shapes = (
        jax.ShapeDtypeStruct((2 * rows, bins), jnp.float32),
        jax.ShapeDtypeStruct((2, 16, 512), jnp.bfloat16),
    )
    return pl.pallas_call(
        kernel,
        out_shape=shapes[:outs],
        in_specs=[VMEM] * len(operands),
        out_specs=(VMEM,) * outs,
        scratch_shapes=[pltpu.VMEM((LANES, 2 * bins - LANES), jnp.bfloat16)],
        compiler_params=pltpu.CompilerParams(vmem_limit_bytes=8 * 2**20),
    )(*operands)


def array_kernel(tab, words, out):
    project_rows(tab, words, out, 0)


ORDER = ((0, 0), (0, 3), (0, 2), (0, 1), (1, 0), (1, 3), (1, 2), (1, 1))


def last_kernel(tab, words, *refs):
    parts, out = refs[:-1], refs[-1]
    x, z_high = lax.axis_index("x"), lax.axis_index("z_hi")
    places = [
        8 * (1 - z_high if far else z_high) + 2 * (x ^ step) for far, step in ORDER
    ]
    for place, part in zip(places, parts):
        out[pl.ds(place, 2)] = part[...]
    project_rows(tab, words, out, places[-1])


def project(kernel, owners, operands):
    return pl.pallas_call(
        kernel,
        out_shape=jax.ShapeDtypeStruct((owners, 16, 512), jnp.bfloat16),
        in_specs=[VMEM] * len(operands),
        out_specs=VMEM,
        compiler_params=pltpu.CompilerParams(vmem_limit_bytes=8 * 2**20),
    )(*operands)


def permuted(array, axis, step, size):
    return lax.ppermute(array, axis, [(i ^ step, i) for i in range(size)])


def image(sinogram, detector_coord):
    slices, angles, bins = sinogram.shape
    width = detector_coord.shape[2]
    core = lax.axis_index("core")

    words = packed(detector_coord).reshape(angles, 2, 2, 2, 3 * LANES)
    keep = lax.dynamic_index_in_dim(words, core, 2, keepdims=False).reshape(8, 3 * LANES)
    give = lax.dynamic_index_in_dim(words, 1 - core, 2, keepdims=False).reshape(8, 3 * LANES)
    own = jnp.stack([keep, permuted(give, "core", 1, 2)])
    other = permuted(own, "z_hi", 1, 2)

    sinos = [sinogram, permuted(sinogram, "core", 1, 2)]
    rows = [sino.reshape(slices * angles, bins) for sino in sinos]
    (early,) = prepared(early_kernel, 1, rows)
    tab, near_0 = prepared(late_kernel, 2, [*rows, own, early])
    near = [own] + [permuted(own, "x", s, 4) for s in (1, 2, 3)]
    other, near_0 = lax.optimization_barrier((other, near_0))
    far = [other] + [permuted(other, "x", s, 4) for s in (1, 2, 3)]
    done = [near_0]
    done += [project(array_kernel, 2, [tab, near[s]]) for s in (3, 2, 1)]
    done += [project(array_kernel, 2, [tab, far[s]]) for s in (0, 3, 2)]
    partial = project(last_kernel, 16, [tab, far[1], *done])
    parts = lax.all_to_all(partial, ("y", "z_lo"), 0, 0, tiled=True)
    scale = jnp.float32(math.pi / (angles * lax.axis_size(("y", "z_lo", "core"))))
    image_rows = jnp.sum(parts.astype(jnp.float32), axis=0) * scale
    return image_rows.reshape(2, slices, width)


def solution(mesh):
    names = ("y", "z_lo", "core", "z_hi", "x")
    fine = Mesh(mesh.devices.reshape(4, 4, 2, 2, 4), names)
    ang, sl = ("y", "z_lo", "core"), ("z_hi", "x")
    in_specs = (P(sl, ang, None), P(ang, sl, None))
    return jax.shard_map(
        image, mesh=fine, in_specs=in_specs, out_specs=P(ang, sl, None), check_vma=False
    )
```

```python
import math

import jax
import jax.numpy as jnp
from jax import lax
from jax.experimental import pallas as pl
from jax.experimental.pallas import tpu as pltpu
from jax.sharding import Mesh
from jax.sharding import PartitionSpec as P

LANES = 128
LANE_DIMS = lax.GatherDimensionNumbers(
    offset_dims=(),
    collapsed_slice_dims=(1,),
    start_index_map=(1,),
    operand_batching_dims=(0,),
    start_indices_batching_dims=(0,),
)
VMEM = pl.BlockSpec(memory_space=pltpu.VMEM)


def lane_gather(table, lanes):
    return lax.gather(
        table, lanes[..., None], LANE_DIMS, (1, 1), mode=lax.GatherScatterMode.PROMISE_IN_BOUNDS
    )


def filter_kernel(own, other, out, strip):
    bins = own.shape[1]
    blocks = bins // LANES
    for j in range(2 * blocks - 1):
        first = lax.broadcasted_iota(jnp.int32, (LANES, LANES), 0)
        second = lax.broadcasted_iota(jnp.int32, (LANES, LANES), 1)
        offset = second - first + (j - blocks + 1) * LANES
        offset_sq = jnp.maximum((offset * offset).astype(jnp.float32), jnp.float32(1.0))
        values = jnp.where(
            (offset & 1) != 0, jnp.float32(-1.0 / math.pi**2) / offset_sq, jnp.float32(0.0)
        )
        if j == blocks - 1:
            values = jnp.where(offset == 0, jnp.float32(0.25), values)
        strip[:, j * LANES : (j + 1) * LANES] = values.astype(jnp.bfloat16)
    rows = jnp.concatenate([own[...], other[...]], axis=0)
    total = None
    for k in range(blocks):
        start = (blocks - 1 - k) * LANES
        part = jnp.dot(
            rows[:, k * LANES : (k + 1) * LANES],
            strip[:, start : start + bins],
            preferred_element_type=jnp.float32,
        )
        total = part if total is None else total + part
    out[...] = total.astype(jnp.bfloat16).astype(jnp.float32)


def transposed(tiles):
    sublane = lax.broadcasted_iota(jnp.int32, (8, LANES), 0)
    for step in (4, 2, 1):
        low = (sublane & step) == 0
        done = list(tiles)
        for i in range(8):
            if not i & step:
                a, b = tiles[i], tiles[i + step]
                done[i] = jnp.where(low, a, pltpu.roll(b, step, 0))
                done[i + step] = jnp.where(low, pltpu.roll(a, 8 - step, 0), b)
        tiles = done
    return tiles


def packed(coords):
    tiles = [coords[..., p * LANES : (p + 1) * LANES] >> 6 for p in range(4)]
    words = [tiles[p] | ((tiles[3] >> (8 * p)) << 24) for p in range(3)]
    return jnp.concatenate(words, axis=-1)


def unpacked(words):
    tiles = [words[:, p * LANES : (p + 1) * LANES] for p in range(3)]
    top = [lax.shift_right_logical(tile, 24) for tile in tiles]
    return [tile & 16777215 for tile in tiles] + [top[0] | (top[1] << 8) | (top[2] << 16)]


def project_rows(tab, words, out, place):
    sublane = lax.broadcasted_iota(jnp.int32, (8, LANES), 0)
    tiles = [unpacked(words[core]) for core in range(2)]
    for p in range(4):
        sums = [None] * 8
        for core in range(2):
            c = tiles[core][p]
            left = c >> 14
            fraction = (c & 16383).astype(jnp.float32) * jnp.float32(1.0 / 16384.0)
            w_left = (1.0 - fraction).astype(jnp.bfloat16).astype(jnp.float32)
            w_right = fraction.astype(jnp.bfloat16).astype(jnp.float32)
            bins = jnp.concatenate([left, left + 1], axis=0).astype(jnp.int16)
            lanes = bins & jnp.int16(LANES - 1)
            high = [(bins & jnp.int16(bit)) != 0 for bit in (128, 256, 512)]
            for s in range(8):
                row = core * 16 + s * 2
                taps = []
                for k in range(8):
                    at = slice(k * LANES, (k + 1) * LANES)
                    source = jnp.where(
                        sublane < 4,
                        jnp.broadcast_to(tab[row : row + 1, at], (8, LANES)),
                        jnp.broadcast_to(tab[row + 1 : row + 2, at], (8, LANES)),
                    )
                    source = jnp.concatenate([source, source], axis=0).astype(jnp.bfloat16)
                    taps.append(lane_gather(source, lanes))
                for mask in high:
                    taps = [jnp.where(mask, taps[k + 1], taps[k]) for k in range(0, len(taps), 2)]
                both = taps[0].astype(jnp.float32)
                part = both[:8] * w_left + both[8:] * w_right
                sums[s] = part if sums[s] is None else sums[s] + part
        rows = transposed([total + pltpu.roll(total, 4, 0) for total in sums])
        for pair in range(2):
            for r in range(2):
                value = rows[pair * 2 + r].astype(out.dtype)
                out[place + pair, r * 8 : (r + 1) * 8, p * LANES : (p + 1) * LANES] = value


def early_kernel(own, other, tab, strip):
    @pl.when(lax.axis_index("z_hi") == 0)
    def _():
        filter_kernel(own, other, tab, strip)


def late_kernel(own, other, words, tab_early, tab, near, strip):
    early = lax.axis_index("z_hi") == 0

    @pl.when(early)
    def _():
        tab[...] = tab_early[...]

    @pl.when(jnp.logical_not(early))
    def _():
        filter_kernel(own, other, tab, strip)

    project_rows(tab, words, near, 0)


def prepared(kernel, outs, operands):
    rows, bins = operands[0].shape
    shapes = (
        jax.ShapeDtypeStruct((2 * rows, bins), jnp.float32),
        jax.ShapeDtypeStruct((2, 16, 512), jnp.bfloat16),
    )
    return pl.pallas_call(
        kernel,
        out_shape=shapes[:outs],
        in_specs=[VMEM] * len(operands),
        out_specs=(VMEM,) * outs,
        scratch_shapes=[pltpu.VMEM((LANES, 2 * bins - LANES), jnp.bfloat16)],
        compiler_params=pltpu.CompilerParams(vmem_limit_bytes=8 * 2**20),
    )(*operands)


def array_kernel(tab, words, out):
    project_rows(tab, words, out, 0)


ORDER = ((0, 0), (0, 3), (0, 1), (1, 0), (1, 3), (1, 1), (0, 2), (1, 2))


def last_kernel(tab, words, *refs):
    parts, out = refs[:-1], refs[-1]
    x, z_high = lax.axis_index("x"), lax.axis_index("z_hi")
    places = [
        8 * (1 - z_high if far else z_high) + 2 * (x ^ step) for far, step in ORDER
    ]
    for place, part in zip(places, parts):
        out[pl.ds(place, 2)] = part[...]
    project_rows(tab, words, out, places[-1])


def project(kernel, owners, operands):
    return pl.pallas_call(
        kernel,
        out_shape=jax.ShapeDtypeStruct((owners, 16, 512), jnp.bfloat16),
        in_specs=[VMEM] * len(operands),
        out_specs=VMEM,
        compiler_params=pltpu.CompilerParams(vmem_limit_bytes=8 * 2**20),
    )(*operands)


def permuted(array, axis, step, size):
    return lax.ppermute(array, axis, [(i ^ step, i) for i in range(size)])


def along_x(array):
    three = permuted(array, "x", 3, 4)
    one = permuted(array, "x", 1, 4)
    return [array, one, permuted(three, "x", 1, 4), three]


def image(sinogram, detector_coord):
    slices, angles, bins = sinogram.shape
    width = detector_coord.shape[2]
    core = lax.axis_index("core")

    words = packed(detector_coord).reshape(angles, 2, 2, 2, 3 * LANES)
    keep = lax.dynamic_index_in_dim(words, core, 2, keepdims=False).reshape(8, 3 * LANES)
    give = lax.dynamic_index_in_dim(words, 1 - core, 2, keepdims=False).reshape(8, 3 * LANES)
    own = jnp.stack([keep, permuted(give, "core", 1, 2)])
    other = permuted(own, "z_hi", 1, 2)

    sinos = [sinogram, permuted(sinogram, "core", 1, 2)]
    rows = [sino.reshape(slices * angles, bins) for sino in sinos]
    (early,) = prepared(early_kernel, 1, rows)
    tab, near_0 = prepared(late_kernel, 2, [*rows, own, early])
    other, near_0 = lax.optimization_barrier((other, near_0))
    near, far = along_x(own), along_x(other)
    done = [near_0]
    done += [project(array_kernel, 2, [tab, near[s]]) for s in (3, 1)]
    done += [project(array_kernel, 2, [tab, far[s]]) for s in (0, 3, 1)]
    done.append(project(array_kernel, 2, [tab, near[2]]))
    partial = project(last_kernel, 16, [tab, far[2], *done])
    parts = lax.all_to_all(partial, ("y", "z_lo"), 0, 0, tiled=True)
    scale = jnp.float32(math.pi / (angles * lax.axis_size(("y", "z_lo", "core"))))
    image_rows = jnp.sum(parts.astype(jnp.float32), axis=0) * scale
    return image_rows.reshape(2, slices, width)


def solution(mesh):
    names = ("y", "z_lo", "core", "z_hi", "x")
    fine = Mesh(mesh.devices.reshape(4, 4, 2, 2, 4), names)
    ang, sl = ("y", "z_lo", "core"), ("z_hi", "x")
    in_specs = (P(sl, ang, None), P(ang, sl, None))
    return jax.shard_map(
        image, mesh=fine, in_specs=in_specs, out_specs=P(ang, sl, None), check_vma=False
    )
```

```python
import math

import jax
import jax.numpy as jnp
from jax import lax
from jax.experimental import pallas as pl
from jax.experimental.pallas import tpu as pltpu
from jax.sharding import Mesh
from jax.sharding import PartitionSpec as P

LANES = 128
LANE_DIMS = lax.GatherDimensionNumbers(
    offset_dims=(),
    collapsed_slice_dims=(1,),
    start_index_map=(1,),
    operand_batching_dims=(0,),
    start_indices_batching_dims=(0,),
)
VMEM = pl.BlockSpec(memory_space=pltpu.VMEM)


def lane_gather(table, lanes):
    return lax.gather(
        table, lanes[..., None], LANE_DIMS, (1, 1), mode=lax.GatherScatterMode.PROMISE_IN_BOUNDS
    )


def filter_kernel(own, other, out, strip):
    bins = own.shape[1]
    blocks = bins // LANES
    for j in range(2 * blocks - 1):
        first = lax.broadcasted_iota(jnp.int32, (LANES, LANES), 0)
        second = lax.broadcasted_iota(jnp.int32, (LANES, LANES), 1)
        offset = second - first + (j - blocks + 1) * LANES
        offset_sq = jnp.maximum((offset * offset).astype(jnp.float32), jnp.float32(1.0))
        values = jnp.where(
            (offset & 1) != 0, jnp.float32(-1.0 / math.pi**2) / offset_sq, jnp.float32(0.0)
        )
        if j == blocks - 1:
            values = jnp.where(offset == 0, jnp.float32(0.25), values)
        strip[:, j * LANES : (j + 1) * LANES] = values.astype(jnp.bfloat16)
    rows = jnp.concatenate([own[...], other[...]], axis=0)
    total = None
    for k in range(blocks):
        start = (blocks - 1 - k) * LANES
        part = jnp.dot(
            rows[:, k * LANES : (k + 1) * LANES],
            strip[:, start : start + bins],
            preferred_element_type=jnp.float32,
        )
        total = part if total is None else total + part
    out[...] = total.astype(jnp.bfloat16).astype(jnp.float32)


def transposed(tiles):
    sublane = lax.broadcasted_iota(jnp.int32, (8, LANES), 0)
    for step in (4, 2, 1):
        low = (sublane & step) == 0
        done = list(tiles)
        for i in range(8):
            if not i & step:
                a, b = tiles[i], tiles[i + step]
                done[i] = jnp.where(low, a, pltpu.roll(b, step, 0))
                done[i + step] = jnp.where(low, pltpu.roll(a, 8 - step, 0), b)
        tiles = done
    return tiles


def packed(coords):
    tiles = [coords[..., p * LANES : (p + 1) * LANES] >> 6 for p in range(4)]
    words = [tiles[p] | ((tiles[3] >> (8 * p)) << 24) for p in range(3)]
    return jnp.concatenate(words, axis=-1)


def unpacked(words):
    tiles = [words[:, p * LANES : (p + 1) * LANES] for p in range(3)]
    top = [lax.shift_right_logical(tile, 24) for tile in tiles]
    return [tile & 16777215 for tile in tiles] + [top[0] | (top[1] << 8) | (top[2] << 16)]


def project_rows(tab, words, out, place):
    sublane = lax.broadcasted_iota(jnp.int32, (8, LANES), 0)
    tiles = [unpacked(words[core]) for core in range(2)]
    for p in range(4):
        sums = [None] * 8
        for core in range(2):
            c = tiles[core][p]
            left = c >> 14
            fraction = (c & 16383).astype(jnp.float32) * jnp.float32(1.0 / 16384.0)
            w_left = (1.0 - fraction).astype(jnp.bfloat16).astype(jnp.float32)
            w_right = fraction.astype(jnp.bfloat16).astype(jnp.float32)
            bins = jnp.concatenate([left, left + 1], axis=0).astype(jnp.int16)
            lanes = bins & jnp.int16(LANES - 1)
            high = [(bins & jnp.int16(bit)) != 0 for bit in (128, 256, 512)]
            for s in range(8):
                row = core * 16 + s * 2
                taps = []
                for k in range(8):
                    at = slice(k * LANES, (k + 1) * LANES)
                    source = jnp.where(
                        sublane < 4,
                        jnp.broadcast_to(tab[row : row + 1, at], (8, LANES)),
                        jnp.broadcast_to(tab[row + 1 : row + 2, at], (8, LANES)),
                    )
                    source = jnp.concatenate([source, source], axis=0).astype(jnp.bfloat16)
                    taps.append(lane_gather(source, lanes))
                for mask in high:
                    taps = [jnp.where(mask, taps[k + 1], taps[k]) for k in range(0, len(taps), 2)]
                both = taps[0].astype(jnp.float32)
                part = both[:8] * w_left + both[8:] * w_right
                sums[s] = part if sums[s] is None else sums[s] + part
        rows = transposed([total + pltpu.roll(total, 4, 0) for total in sums])
        for pair in range(2):
            for r in range(2):
                value = rows[pair * 2 + r].astype(out.dtype)
                out[place + pair, r * 8 : (r + 1) * 8, p * LANES : (p + 1) * LANES] = value


def early_kernel(own, other, tab, strip):
    @pl.when(lax.axis_index("z_hi") == 0)
    def _():
        filter_kernel(own, other, tab, strip)


def late_kernel(own, other, words, tab_early, tab, near, strip):
    early = lax.axis_index("z_hi") == 0

    @pl.when(early)
    def _():
        tab[...] = tab_early[...]

    @pl.when(jnp.logical_not(early))
    def _():
        filter_kernel(own, other, tab, strip)

    project_rows(tab, words, near, 0)


def prepared(kernel, outs, operands):
    rows, bins = operands[0].shape
    shapes = (
        jax.ShapeDtypeStruct((2 * rows, bins), jnp.float32),
        jax.ShapeDtypeStruct((2, 16, 512), jnp.bfloat16),
    )
    return pl.pallas_call(
        kernel,
        out_shape=shapes[:outs],
        in_specs=[VMEM] * len(operands),
        out_specs=(VMEM,) * outs,
        scratch_shapes=[pltpu.VMEM((LANES, 2 * bins - LANES), jnp.bfloat16)],
        compiler_params=pltpu.CompilerParams(vmem_limit_bytes=8 * 2**20),
    )(*operands)


def array_kernel(tab, words, out):
    project_rows(tab, words, out, 0)


ORDER = ((0, 0), (0, 3), (0, 1), (1, 0), (1, 2), (1, 3), (1, 1), (0, 2))


def last_kernel(tab, words, *refs):
    parts, out = refs[:-1], refs[-1]
    x, z_high = lax.axis_index("x"), lax.axis_index("z_hi")
    places = [
        8 * (1 - z_high if far else z_high) + 2 * (x ^ step) for far, step in ORDER
    ]
    for place, part in zip(places, parts):
        out[pl.ds(place, 2)] = part[...]
    project_rows(tab, words, out, places[-1])


def project(kernel, owners, operands):
    return pl.pallas_call(
        kernel,
        out_shape=jax.ShapeDtypeStruct((owners, 16, 512), jnp.bfloat16),
        in_specs=[VMEM] * len(operands),
        out_specs=VMEM,
        compiler_params=pltpu.CompilerParams(vmem_limit_bytes=8 * 2**20),
    )(*operands)


def permuted(array, axis, step, size):
    return lax.ppermute(array, axis, [(i ^ step, i) for i in range(size)])


def image(sinogram, detector_coord):
    slices, angles, bins = sinogram.shape
    width = detector_coord.shape[2]
    core = lax.axis_index("core")

    words = packed(detector_coord).reshape(angles, 2, 2, 2, 3 * LANES)
    keep = lax.dynamic_index_in_dim(words, core, 2, keepdims=False).reshape(8, 3 * LANES)
    give = lax.dynamic_index_in_dim(words, 1 - core, 2, keepdims=False).reshape(8, 3 * LANES)
    own = jnp.stack([keep, permuted(give, "core", 1, 2)])
    other = permuted(own, "z_hi", 1, 2)

    sinos = [sinogram, permuted(sinogram, "core", 1, 2)]
    rows = [sino.reshape(slices * angles, bins) for sino in sinos]
    (early,) = prepared(early_kernel, 1, rows)
    tab, near_0 = prepared(late_kernel, 2, [*rows, own, early])
    other, near_0 = lax.optimization_barrier((other, near_0))
    near_3, near_1 = (permuted(own, "x", s, 4) for s in (3, 1))
    near = [own, near_1, permuted(near_3, "x", 1, 4), near_3]
    far = [other] + [permuted(other, "x", s, 4) for s in (1, 2, 3)]
    done = [near_0]
    done += [project(array_kernel, 2, [tab, near[s]]) for s in (3, 1)]
    done += [project(array_kernel, 2, [tab, far[s]]) for s in (0, 2, 3, 1)]
    partial = project(last_kernel, 16, [tab, near[2], *done])
    parts = lax.all_to_all(partial, ("y", "z_lo"), 0, 0, tiled=True)
    scale = jnp.float32(math.pi / (angles * lax.axis_size(("y", "z_lo", "core"))))
    image_rows = jnp.sum(parts.astype(jnp.float32), axis=0) * scale
    return image_rows.reshape(2, slices, width)


def solution(mesh):
    names = ("y", "z_lo", "core", "z_hi", "x")
    fine = Mesh(mesh.devices.reshape(4, 4, 2, 2, 4), names)
    ang, sl = ("y", "z_lo", "core"), ("z_hi", "x")
    in_specs = (P(sl, ang, None), P(ang, sl, None))
    return jax.shard_map(
        image, mesh=fine, in_specs=in_specs, out_specs=P(ang, sl, None), check_vma=False
    )
```

```python
import math

import jax
import jax.numpy as jnp
from jax import lax
from jax.experimental import pallas as pl
from jax.experimental.pallas import tpu as pltpu
from jax.sharding import Mesh
from jax.sharding import PartitionSpec as P

LANES = 128
LANE_DIMS = lax.GatherDimensionNumbers(
    offset_dims=(),
    collapsed_slice_dims=(1,),
    start_index_map=(1,),
    operand_batching_dims=(0,),
    start_indices_batching_dims=(0,),
)
VMEM = pl.BlockSpec(memory_space=pltpu.VMEM)


def lane_gather(table, lanes):
    return lax.gather(
        table, lanes[..., None], LANE_DIMS, (1, 1), mode=lax.GatherScatterMode.PROMISE_IN_BOUNDS
    )


def filter_kernel(own, other, out, strip):
    bins = own.shape[1]
    blocks = bins // LANES
    for j in range(2 * blocks - 1):
        first = lax.broadcasted_iota(jnp.int32, (LANES, LANES), 0)
        second = lax.broadcasted_iota(jnp.int32, (LANES, LANES), 1)
        offset = second - first + (j - blocks + 1) * LANES
        offset_sq = jnp.maximum((offset * offset).astype(jnp.float32), jnp.float32(1.0))
        values = jnp.where(
            (offset & 1) != 0, jnp.float32(-1.0 / math.pi**2) / offset_sq, jnp.float32(0.0)
        )
        if j == blocks - 1:
            values = jnp.where(offset == 0, jnp.float32(0.25), values)
        strip[:, j * LANES : (j + 1) * LANES] = values.astype(jnp.bfloat16)
    rows = jnp.concatenate([own[...], other[...]], axis=0)
    total = None
    for k in range(blocks):
        start = (blocks - 1 - k) * LANES
        part = jnp.dot(
            rows[:, k * LANES : (k + 1) * LANES],
            strip[:, start : start + bins],
            preferred_element_type=jnp.float32,
        )
        total = part if total is None else total + part
    out[...] = total.astype(jnp.bfloat16).astype(jnp.float32)


def transposed(tiles):
    sublane = lax.broadcasted_iota(jnp.int32, (8, LANES), 0)
    for step in (4, 2, 1):
        low = (sublane & step) == 0
        done = list(tiles)
        for i in range(8):
            if not i & step:
                a, b = tiles[i], tiles[i + step]
                done[i] = jnp.where(low, a, pltpu.roll(b, step, 0))
                done[i + step] = jnp.where(low, pltpu.roll(a, 8 - step, 0), b)
        tiles = done
    return tiles


def packed(coords):
    tiles = [coords[..., p * LANES : (p + 1) * LANES] >> 6 for p in range(4)]
    words = [tiles[p] | ((tiles[3] >> (8 * p)) << 24) for p in range(3)]
    return jnp.concatenate(words, axis=-1)


def unpacked(words):
    tiles = [words[:, p * LANES : (p + 1) * LANES] for p in range(3)]
    top = [lax.shift_right_logical(tile, 24) for tile in tiles]
    return [tile & 16777215 for tile in tiles] + [top[0] | (top[1] << 8) | (top[2] << 16)]


def project_rows(tab, words, out, place):
    sublane = lax.broadcasted_iota(jnp.int32, (8, LANES), 0)
    tiles = [unpacked(words[core]) for core in range(2)]
    for p in range(4):
        sums = [None] * 8
        for core in range(2):
            c = tiles[core][p]
            left = c >> 14
            fraction = (c & 16383).astype(jnp.float32) * jnp.float32(1.0 / 16384.0)
            w_left = (1.0 - fraction).astype(jnp.bfloat16).astype(jnp.float32)
            w_right = fraction.astype(jnp.bfloat16).astype(jnp.float32)
            bins = jnp.concatenate([left, left + 1], axis=0).astype(jnp.int16)
            lanes = bins & jnp.int16(LANES - 1)
            high = [(bins & jnp.int16(bit)) != 0 for bit in (128, 256, 512)]
            for s in range(8):
                row = core * 16 + s * 2
                taps = []
                for k in range(8):
                    at = slice(k * LANES, (k + 1) * LANES)
                    source = jnp.where(
                        sublane < 4,
                        jnp.broadcast_to(tab[row : row + 1, at], (8, LANES)),
                        jnp.broadcast_to(tab[row + 1 : row + 2, at], (8, LANES)),
                    )
                    source = jnp.concatenate([source, source], axis=0).astype(jnp.bfloat16)
                    taps.append(lane_gather(source, lanes))
                for mask in high:
                    taps = [jnp.where(mask, taps[k + 1], taps[k]) for k in range(0, len(taps), 2)]
                both = taps[0].astype(jnp.float32)
                part = both[:8] * w_left + both[8:] * w_right
                sums[s] = part if sums[s] is None else sums[s] + part
        rows = transposed([total + pltpu.roll(total, 4, 0) for total in sums])
        for pair in range(2):
            for r in range(2):
                value = rows[pair * 2 + r].astype(out.dtype)
                out[place + pair, r * 8 : (r + 1) * 8, p * LANES : (p + 1) * LANES] = value


def prepare_kernel(own, other, words, tab, near, strip):
    filter_kernel(own, other, tab, strip)
    project_rows(tab, words, near, 0)


def prepared(kernel, outs, operands):
    rows, bins = operands[0].shape
    shapes = (
        jax.ShapeDtypeStruct((2 * rows, bins), jnp.float32),
        jax.ShapeDtypeStruct((2, 16, 512), jnp.bfloat16),
    )
    return pl.pallas_call(
        kernel,
        out_shape=shapes[:outs],
        in_specs=[VMEM] * len(operands),
        out_specs=(VMEM,) * outs,
        scratch_shapes=[pltpu.VMEM((LANES, 2 * bins - LANES), jnp.bfloat16)],
        compiler_params=pltpu.CompilerParams(vmem_limit_bytes=8 * 2**20),
    )(*operands)


def array_kernel(tab, words, out):
    project_rows(tab, words, out, 0)


ORDER = ((0, 0), (0, 3), (0, 1), (1, 0), (1, 3), (1, 1), (0, 2), (1, 2))


def last_kernel(tab, words, *refs):
    parts, out = refs[:-1], refs[-1]
    x, z_high = lax.axis_index("x"), lax.axis_index("z_hi")
    places = [
        8 * (1 - z_high if far else z_high) + 2 * (x ^ step) for far, step in ORDER
    ]
    for place, part in zip(places, parts):
        out[pl.ds(place, 2)] = part[...]
    project_rows(tab, words, out, places[-1])


def project(kernel, owners, operands):
    return pl.pallas_call(
        kernel,
        out_shape=jax.ShapeDtypeStruct((owners, 16, 512), jnp.bfloat16),
        in_specs=[VMEM] * len(operands),
        out_specs=VMEM,
        compiler_params=pltpu.CompilerParams(vmem_limit_bytes=8 * 2**20),
    )(*operands)


def permuted(array, axis, step, size):
    return lax.ppermute(array, axis, [(i ^ step, i) for i in range(size)])


def along_x(array):
    three = permuted(array, "x", 3, 4)
    one = permuted(array, "x", 1, 4)
    return [array, one, permuted(three, "x", 1, 4), three]


def image(sinogram, detector_coord):
    slices, angles, bins = sinogram.shape
    width = detector_coord.shape[2]
    core = lax.axis_index("core")

    words = packed(detector_coord).reshape(angles, 2, 2, 2, 3 * LANES)
    keep = lax.dynamic_index_in_dim(words, core, 2, keepdims=False).reshape(8, 3 * LANES)
    give = lax.dynamic_index_in_dim(words, 1 - core, 2, keepdims=False).reshape(8, 3 * LANES)
    own = jnp.stack([keep, permuted(give, "core", 1, 2)])
    other = permuted(own, "z_hi", 1, 2)

    sinos = [sinogram, permuted(sinogram, "core", 1, 2)]
    rows = [sino.reshape(slices * angles, bins) for sino in sinos]
    tab, near_0 = prepared(prepare_kernel, 2, [*rows, own])
    other, near_0 = lax.optimization_barrier((other, near_0))
    near, far = along_x(own), along_x(other)
    done = [near_0]
    done += [project(array_kernel, 2, [tab, near[s]]) for s in (3, 1)]
    done += [project(array_kernel, 2, [tab, far[s]]) for s in (0, 3, 1)]
    done.append(project(array_kernel, 2, [tab, near[2]]))
    partial = project(last_kernel, 16, [tab, far[2], *done])
    parts = lax.all_to_all(partial, ("y", "z_lo"), 0, 0, tiled=True)
    scale = jnp.float32(math.pi / (angles * lax.axis_size(("y", "z_lo", "core"))))
    image_rows = jnp.sum(parts.astype(jnp.float32), axis=0) * scale
    return image_rows.reshape(2, slices, width)


def solution(mesh):
    names = ("y", "z_lo", "core", "z_hi", "x")
    fine = Mesh(mesh.devices.reshape(4, 4, 2, 2, 4), names)
    ang, sl = ("y", "z_lo", "core"), ("z_hi", "x")
    in_specs = (P(sl, ang, None), P(ang, sl, None))
    return jax.shard_map(
        image, mesh=fine, in_specs=in_specs, out_specs=P(ang, sl, None), check_vma=False
    )
```
